32 devices in a mesh: seq: 16 (over z, y, core), sub: 2 (over x).
Axes of the slice: x: 2, y: 2, z: 4, core: 2. Of those that a mesh axis runs over, the one named last changes fastest.
Arguments:
- tokens: bfloat16 [4096, 1024], P(('seq', 'sub')), may hold values from -6 to 6
- cotangent: bfloat16 [4096, 1024], P(('seq', 'sub')), may hold values from -6 to 6
- fine_qkv: bfloat16 [1024, 3, 1024], replicated, may hold values from -0.1875 to 0.1875
- fine_out: bfloat16 [1024, 1024], replicated, may hold values from -0.1875 to 0.1875
- coarse_qkv: bfloat16 [1024, 3, 1024], P(None, None, 'sub'), may hold values from -0.1875 to 0.1875
- coarse_out: bfloat16 [1024, 1024], P('sub'), may hold values from -0.5 to 0.5
Outputs:
- output: bfloat16 [4096, 1024], P(('seq', 'sub'))
- grad_tokens: bfloat16 [4096, 1024], P(('seq', 'sub'))
The draws below stay inside these ranges and needn't reach their ends.
All inputs are finite; a program needn't handle non-finite values.
Results may differ from the reference program's by a relative error of at most 0.02.
Values may be sent and summed in bfloat16 or wider, within the bound.
A program may use at most 128 MiB of HBM per device.

```python
import jax
import jax.numpy as jnp
from jax import lax

D = 1024
HEADS = 16
HEAD_DIM = 64
WINDOW = 512
POOL = 16
SEQ_LEN = 4096


def level_of(key, dims, cuts, low, top_value):
    factor_of, own = 1.0, jax.random.fold_in(key, 6)
    for axis_at, parts in cuts:
        steps = jnp.exp(jax.random.uniform(jax.random.fold_in(own, axis_at), (parts,), jnp.float32, low / len(cuts), top_value / len(cuts)))
        factor_of = factor_of * jnp.repeat(steps, dims[axis_at] // parts).reshape([-1 if axis == axis_at else 1 for axis in range(len(dims))])
    return factor_of


def normal_values(key, shape, deviation, bound, shards=(), kind=jnp.bfloat16):
    entries = deviation * jax.random.normal(key, shape, jnp.float32)
    if shards:
        entries = entries * level_of(key, shape, shards, -0.22, 0.18)
    return jnp.clip(entries, -bound, bound).astype(kind)


def setup_inputs(seed: int = 0) -> dict:
    splits = jax.random.split(jax.random.key(seed), 7)
    tokens = normal_values(splits[0], (SEQ_LEN, D), 1.0, 6.0, ((0, 32),))
    cotangent = normal_values(splits[1], (SEQ_LEN, D), 1.0, 6.0, ((0, 32),))
    fine_qkv = normal_values(splits[2], (D, 3, D), D ** -0.5, 0.1875)
    fine_out = normal_values(splits[3], (D, D), D ** -0.5, 0.1875)
    coarse_qkv = normal_values(splits[4], (D, 3, D), D ** -0.5, 0.1875, ((2, 2),))
    coarse_out = normal_values(splits[5], (D, D), (D // 8) ** -0.5, 0.5, ((0, 2),))
    return {"tokens": tokens, "cotangent": cotangent, "fine_qkv": fine_qkv, "fine_out": fine_out, "coarse_qkv": coarse_qkv, "coarse_out": coarse_out}


EPS = 1e-06

def rms_rows(values):
    widened = values.astype(jnp.float32)
    factor = lax.rsqrt(lax.optimization_barrier(jnp.mean(widened * widened, axis=-1, keepdims=True)) + EPS)
    return (widened * factor, factor)

def norm_back(grad_rows, normed, factor):
    return factor * (grad_rows - normed * lax.optimization_barrier(jnp.mean(normed * grad_rows, axis=-1, keepdims=True)))

def project_rows(normed_b, weight):
    row_count = normed_b.shape[0]
    local_width = weight.shape[2]
    projected = jnp.dot(normed_b, weight.reshape(weight.shape[0], 3 * local_width), preferred_element_type=jnp.float32)
    projected = projected.reshape(row_count, 3, local_width // HEAD_DIM, HEAD_DIM)
    query_unit, query_scale = rms_rows(projected[:, 0])
    key_unit, key_scale = rms_rows(projected[:, 1])
    return (query_unit, query_scale, key_unit, key_scale, projected[:, 2])

def fdot(spec, left, right):
    return jnp.einsum(spec, left.astype(jnp.float32), right.astype(jnp.float32), precision=lax.Precision.HIGHEST)

def window_exp(query_blk, key_blk, first_pos):
    scores = fdot('qhd,khd->hqk', query_blk, key_blk) * HEAD_DIM ** (-0.5)
    query_pos = lax.broadcasted_iota(jnp.int32, (query_blk.shape[0], key_blk.shape[0]), 0)
    key_pos = lax.broadcasted_iota(jnp.int32, (query_blk.shape[0], key_blk.shape[0]), 1)
    gap = WINDOW + query_pos - key_pos
    allowed = (gap >= 0) & (gap < WINDOW) & (first_pos - WINDOW + key_pos >= 0)
    return jnp.where(allowed[None], jnp.exp(scores), 0.0)

def padded_front(rows):
    return jnp.concatenate([jnp.zeros((WINDOW,) + rows.shape[1:], rows.dtype), rows])

def window_forward(queries, key_rows, value_rows):
    total_len = queries.shape[0]
    key_pad = padded_front(key_rows)
    value_pad = padded_front(value_rows)

    def one_block(block_index):
        first_pos = block_index * WINDOW
        query_blk = lax.dynamic_slice_in_dim(queries, first_pos, WINDOW)
        key_blk = lax.dynamic_slice_in_dim(key_pad, first_pos, 2 * WINDOW)
        value_blk = lax.dynamic_slice_in_dim(value_pad, first_pos, 2 * WINDOW)
        numer = window_exp(query_blk, key_blk, first_pos)
        totals = lax.optimization_barrier(jnp.sum(numer, axis=-1))
        probs_half = (numer / totals[:, :, None]).astype(jnp.bfloat16)
        attended = fdot('hqk,khd->qhd', probs_half, value_blk).astype(jnp.bfloat16)
        return (attended, totals)
    attended, totals = lax.map(one_block, jnp.arange(total_len // WINDOW, dtype=jnp.int32))
    return (attended.reshape(queries.shape), totals)

def window_query_grads(queries, key_rows, value_rows, grad_out, totals, deltas):
    total_len = queries.shape[0]
    key_pad = padded_front(key_rows)
    value_pad = padded_front(value_rows)

    def one_block(inputs):
        block_index, block_totals = inputs
        first_pos = block_index * WINDOW
        query_blk = lax.dynamic_slice_in_dim(queries, first_pos, WINDOW)
        key_blk = lax.dynamic_slice_in_dim(key_pad, first_pos, 2 * WINDOW)
        value_blk = lax.dynamic_slice_in_dim(value_pad, first_pos, 2 * WINDOW)
        grad_blk = lax.dynamic_slice_in_dim(grad_out, first_pos, WINDOW)
        delta_blk = lax.dynamic_slice_in_dim(deltas, first_pos, WINDOW)
        probs_full = window_exp(query_blk, key_blk, first_pos) / block_totals[:, :, None]
        prob_grad = fdot('qhd,khd->hqk', grad_blk, value_blk)
        dscore = (probs_full * (prob_grad - delta_blk.T[:, :, None])).astype(jnp.bfloat16)
        return fdot('hqk,khd->qhd', dscore, key_blk) * HEAD_DIM ** (-0.5)
    grads = lax.map(one_block, (jnp.arange(total_len // WINDOW, dtype=jnp.int32), totals))
    return grads.reshape(queries.shape)

def window_key_grads(queries, key_rows, value_rows, grad_out, totals_rows, deltas):
    total_len = queries.shape[0]
    query_pad = jnp.concatenate([queries, jnp.zeros((WINDOW,) + queries.shape[1:], queries.dtype)])
    grad_pad = jnp.concatenate([grad_out, jnp.zeros((WINDOW,) + grad_out.shape[1:], grad_out.dtype)])
    total_pad = jnp.concatenate([totals_rows, jnp.ones((WINDOW, totals_rows.shape[1]), jnp.float32)])
    delta_pad = jnp.concatenate([deltas, jnp.zeros((WINDOW, deltas.shape[1]), jnp.float32)])

    def one_block(block_index):
        first_key = block_index * WINDOW
        key_blk = lax.dynamic_slice_in_dim(key_rows, first_key, WINDOW)
        value_blk = lax.dynamic_slice_in_dim(value_rows, first_key, WINDOW)
        query_blk = lax.dynamic_slice_in_dim(query_pad, first_key, 2 * WINDOW)
        grad_blk = lax.dynamic_slice_in_dim(grad_pad, first_key, 2 * WINDOW)
        total_blk = lax.dynamic_slice_in_dim(total_pad, first_key, 2 * WINDOW)
        delta_blk = lax.dynamic_slice_in_dim(delta_pad, first_key, 2 * WINDOW)
        scores = fdot('qhd,khd->hqk', query_blk, key_blk) * HEAD_DIM ** (-0.5)
        query_pos = lax.broadcasted_iota(jnp.int32, (2 * WINDOW, WINDOW), 0)
        key_pos = lax.broadcasted_iota(jnp.int32, (2 * WINDOW, WINDOW), 1)
        gap = query_pos - key_pos
        allowed = (gap >= 0) & (gap < WINDOW) & (first_key + query_pos < total_len)
        numer = jnp.where(allowed[None], jnp.exp(scores), 0.0)
        probs_full = numer / total_blk.T[:, :, None]
        probs_half = probs_full.astype(jnp.bfloat16)
        prob_grad = fdot('qhd,khd->hqk', grad_blk, value_blk)
        dscore = (probs_full * (prob_grad - delta_blk.T[:, :, None])).astype(jnp.bfloat16)
        key_grad = fdot('hqk,qhd->khd', dscore, query_blk) * HEAD_DIM ** (-0.5)
        value_grad = fdot('hqk,qhd->khd', probs_half, grad_blk)
        return (key_grad, value_grad)
    key_grad, value_grad = lax.map(one_block, jnp.arange(total_len // WINDOW, dtype=jnp.int32))
    return (key_grad.reshape(key_rows.shape), value_grad.reshape(value_rows.shape))

def coarse_head(head_inputs):
    queries, key_rows, value_rows = head_inputs
    length = queries.shape[0]
    scores = jnp.dot(queries, key_rows.T, preferred_element_type=jnp.float32) * HEAD_DIM ** (-0.5)
    query_pos = lax.broadcasted_iota(jnp.int32, (length, length), 0)
    key_pos = lax.broadcasted_iota(jnp.int32, (length, length), 1)
    numer = jnp.where(key_pos <= query_pos, jnp.exp(scores), 0.0)
    totals = lax.optimization_barrier(jnp.sum(numer, axis=-1))
    probs_half = (numer / totals[:, None]).astype(jnp.bfloat16)
    attended = jnp.dot(probs_half, value_rows, preferred_element_type=jnp.float32).astype(jnp.bfloat16)
    return (attended, totals)

def coarse_head_back(head_inputs):
    queries, key_rows, value_rows, attended, grad_out, totals = head_inputs
    length = queries.shape[0]
    scores = jnp.dot(queries, key_rows.T, preferred_element_type=jnp.float32) * HEAD_DIM ** (-0.5)
    query_pos = lax.broadcasted_iota(jnp.int32, (length, length), 0)
    key_pos = lax.broadcasted_iota(jnp.int32, (length, length), 1)
    numer = jnp.where(key_pos <= query_pos, jnp.exp(scores), 0.0)
    probs_full = numer / totals[:, None]
    probs_half = probs_full.astype(jnp.bfloat16)
    deltas = lax.optimization_barrier(jnp.sum(grad_out.astype(jnp.float32) * attended.astype(jnp.float32), axis=-1))
    prob_grad = jnp.dot(grad_out, value_rows.T, preferred_element_type=jnp.float32)
    dscore = (probs_full * (prob_grad - deltas[:, None])).astype(jnp.bfloat16)
    query_grad = jnp.dot(dscore, key_rows, preferred_element_type=jnp.float32) * HEAD_DIM ** (-0.5)
    key_grad = jnp.dot(dscore.T, queries, preferred_element_type=jnp.float32) * HEAD_DIM ** (-0.5)
    value_grad = jnp.dot(probs_half.T, grad_out, preferred_element_type=jnp.float32)
    return (query_grad, key_grad, value_grad)

def contract_last(left, right):
    return lax.dot_general(left, right, (((1,), (1,)), ((), ())), preferred_element_type=jnp.float32)

def reference(tokens, cotangent, fine_qkv, fine_out, coarse_qkv, coarse_out):
    total_len = tokens.shape[0]
    lead_rows = POOL - 1
    coarse_len = total_len // POOL
    normed_fine, scale_fine = rms_rows(tokens)
    query_unit1, query_scale1, key_unit1, key_scale1, value_raw1 = project_rows(normed_fine.astype(jnp.bfloat16), fine_qkv)
    query_one = query_unit1.astype(jnp.bfloat16)
    key_one = key_unit1.astype(jnp.bfloat16)
    value_one = value_raw1.astype(jnp.bfloat16)
    attended_one, totals_one = window_forward(query_one, key_one, value_one)
    hidden = (tokens.astype(jnp.float32) + jnp.dot(attended_one.reshape(total_len, D), fine_out, preferred_element_type=jnp.float32)).astype(jnp.bfloat16)
    shifted = jnp.concatenate([jnp.zeros((lead_rows, D), jnp.bfloat16), hidden[:total_len - lead_rows]])
    pooled = shifted.reshape(coarse_len, POOL, D).astype(jnp.float32).mean(axis=1).astype(jnp.bfloat16)
    normed_coarse, scale_coarse = rms_rows(pooled)
    query_unit2, query_scale2, key_unit2, key_scale2, value_raw2 = project_rows(normed_coarse.astype(jnp.bfloat16), coarse_qkv)
    query_two = jnp.transpose(query_unit2.astype(jnp.bfloat16), (1, 0, 2))
    key_two = jnp.transpose(key_unit2.astype(jnp.bfloat16), (1, 0, 2))
    value_two = jnp.transpose(value_raw2.astype(jnp.bfloat16), (1, 0, 2))
    attended_two, totals_two = lax.map(coarse_head, (query_two, key_two, value_two))
    attended_rows = jnp.transpose(attended_two, (1, 0, 2)).reshape(coarse_len, D)
    coarse_state = (pooled.astype(jnp.float32) + jnp.dot(attended_rows, coarse_out, preferred_element_type=jnp.float32)).astype(jnp.bfloat16)
    output = (hidden.astype(jnp.float32) + jnp.repeat(coarse_state, POOL, axis=0).astype(jnp.float32)).astype(jnp.bfloat16)
    grad_rows = cotangent.astype(jnp.float32)
    coarse_grad = grad_rows.reshape(coarse_len, POOL, D).sum(axis=1)
    grad_att2 = contract_last(coarse_grad.astype(jnp.bfloat16), coarse_out).astype(jnp.bfloat16)
    grad_att2 = jnp.transpose(grad_att2.reshape(coarse_len, HEADS, HEAD_DIM), (1, 0, 2))
    query_grad2, key_grad2, value_grad2 = lax.map(coarse_head_back, (query_two, key_two, value_two, attended_two, grad_att2, totals_two))
    query_grad2 = norm_back(jnp.transpose(query_grad2, (1, 0, 2)), query_unit2, query_scale2)
    key_grad2 = norm_back(jnp.transpose(key_grad2, (1, 0, 2)), key_unit2, key_scale2)
    value_grad2 = jnp.transpose(value_grad2, (1, 0, 2))
    qkv_grad2 = jnp.stack([query_grad2, key_grad2, value_grad2], axis=1).astype(jnp.bfloat16).reshape(coarse_len, 3 * D)
    normed_grad2 = contract_last(qkv_grad2, coarse_qkv.reshape(D, 3 * D))
    pooled_grad = coarse_grad + norm_back(normed_grad2, normed_coarse, scale_coarse)
    spread = jnp.repeat(pooled_grad / POOL, POOL, axis=0)
    hidden_grad = grad_rows + jnp.concatenate([spread[lead_rows:], jnp.zeros((lead_rows, D), jnp.float32)])
    grad_att1 = contract_last(hidden_grad.astype(jnp.bfloat16), fine_out).astype(jnp.bfloat16).reshape(total_len, HEADS, HEAD_DIM)
    deltas_one = lax.optimization_barrier(jnp.sum(grad_att1.astype(jnp.float32) * attended_one.astype(jnp.float32), axis=-1))
    totals_rows = jnp.transpose(totals_one, (0, 2, 1)).reshape(total_len, HEADS)
    query_grad1 = window_query_grads(query_one, key_one, value_one, grad_att1, totals_one, deltas_one)
    key_grad1, value_grad1 = window_key_grads(query_one, key_one, value_one, grad_att1, totals_rows, deltas_one)
    query_grad1 = norm_back(query_grad1, query_unit1, query_scale1)
    key_grad1 = norm_back(key_grad1, key_unit1, key_scale1)
    qkv_grad1 = jnp.stack([query_grad1, key_grad1, value_grad1], axis=1).astype(jnp.bfloat16).reshape(total_len, 3 * D)
    normed_grad1 = contract_last(qkv_grad1, fine_qkv.reshape(D, 3 * D))
    grad_tokens = (hidden_grad + norm_back(normed_grad1, normed_fine, scale_fine)).astype(jnp.bfloat16)
    return (output, grad_tokens)
```

```python
import functools
import math

import jax
import jax.numpy as jnp
from jax import lax
from jax.experimental import pallas as pl
from jax.experimental.pallas import tpu as pltpu
from jax.sharding import PartitionSpec as P

D = 1024
HEADS = 16
HEAD_DIM = 64
WINDOW = 512
POOL = 16
EPS = 1e-06
F32 = jnp.float32
BF16 = jnp.bfloat16
MESH = pl.DeviceIdType.MESH
PAIR = 2 * HEAD_DIM
SCALE = HEAD_DIM ** (-0.5)
LN2 = math.log(2.0)
QUERY = SCALE / LN2
VMEM = pl.BlockSpec(memory_space=pltpu.VMEM)
ANY = pl.BlockSpec(memory_space=pl.ANY)
SMEM = pl.BlockSpec(memory_space=pltpu.SMEM)


def dot(a, b):
    return jnp.dot(a, b, preferred_element_type=F32)


def dot_nt(a, b):
    return lax.dot_general(a, b, (((1,), (1,)), ((), ())), preferred_element_type=F32)


def dot_tn(a, b):
    return lax.dot_general(a, b, (((0,), (0,)), ((), ())), preferred_element_type=F32)


def split(x):
    hi = x.astype(BF16)
    return hi, (x - hi.astype(F32)).astype(BF16)


def iota(shape, axis):
    return lax.broadcasted_iota(jnp.int32, shape, axis)


def head_sum(x):
    group = (iota((x.shape[1], 128), 0) // HEAD_DIM == iota((x.shape[1], 128), 1)).astype(F32).astype(BF16)
    hi, lo = split(x)
    return dot(hi, group) + dot(lo, group)


def head_mean(x):
    group = iota((PAIR, PAIR), 0) // HEAD_DIM == iota((PAIR, PAIR), 1) // HEAD_DIM
    group = jnp.where(group, 1.0 / HEAD_DIM, 0.0).astype(BF16)
    x = x.astype(BF16)
    return jnp.concatenate([dot(x[:, c : c + PAIR], group) for c in range(0, x.shape[1], PAIR)], axis=1)


def head_rms(raw):
    factor = lax.rsqrt(head_mean(raw * raw) + EPS)
    return raw * factor, factor


def head_back(grad, unit, factor):
    return factor * (grad - unit * head_mean(unit * grad))


def rms_rows(x):
    factor = lax.rsqrt(jnp.mean(x * x, axis=-1, keepdims=True) + EPS)
    return x * factor, factor


def row_back(grad, normed, factor):
    return factor * (grad - normed * jnp.mean(normed * grad, axis=-1, keepdims=True))


def both(pair):
    low = iota(pair.shape, 1) < HEAD_DIM
    wide = pair.astype(F32)
    return jnp.concatenate([jnp.where(low, wide, 0.0), jnp.where(low, 0.0, wide)]).astype(BF16)


def pick(stacked):
    half = stacked.shape[0] // 2
    low = iota((half, PAIR), 1) < HEAD_DIM
    return jnp.where(low, stacked[:half], stacked[half:])


def place():
    subs = lax.axis_size("sub")
    count = lax.axis_size("seq") * subs
    me = lax.axis_index("seq") * subs + lax.axis_index("sub")
    return me, count, subs


def coords(index, subs):
    return (index // subs, index % subs)


def greet_all():
    me, count, subs = place()
    barrier = pltpu.get_barrier_semaphore()

    @pl.loop(1, count)
    def _(k):
        pl.semaphore_signal(
            barrier, inc=1, device_id=coords((me + k) % count, subs), device_id_type=MESH
        )


def met_all():
    pl.semaphore_wait(pltpu.get_barrier_semaphore(), lax.axis_size("seq") * lax.axis_size("sub") - 1)


def remote(src, dst, send, recv, target, subs):
    return pltpu.make_async_remote_copy(
        src_ref=src, dst_ref=dst, send_sem=send, recv_sem=recv,
        device_id=coords(target, subs), device_id_type=MESH,
    )


class Spread:
    def __init__(self, src, dst, out_sem, mid_sem, last_sem, sent):
        self.me, self.count, self.subs = place()
        self.cores = 2 if lax.axis_size("seq") % 2 == 0 else 1
        self.groups = self.count // self.subs // self.cores
        self.sub = self.me % self.subs
        self.core = self.me // self.subs % self.cores
        self.group = self.me // self.subs // self.cores
        self.src, self.dst, self.sems, self.sent = src, dst, (out_sem, mid_sem, last_sem), sent

    def index(self, k, core, j):
        group = (self.group + self.groups - k) % self.groups
        sub = (self.sub + self.subs - j) % self.subs
        return (group * self.cores + (self.core + core) % self.cores) * self.subs + sub

    def copy(self, phase, j, k):
        if phase == 0:
            spot, source = self.me, self.src
            target, sem = self.index(self.groups - k, 0, 0), self.sems[0].at[k]
        elif phase == 1:
            spot = self.index(k, 0, 0)
            target, sem = self.index(0, 0, self.subs - j), self.sems[1].at[j, k]
        else:
            spot = self.index(k, 0, j)
            target, sem = self.index(0, 1, 0), self.sems[2].at[j, k]
        source = self.src if phase == 0 else self.dst.at[spot]
        return remote(source, self.dst.at[spot], self.sent.at[phase, j, k], sem, target, self.subs)

    def arrive(self, phase, j, k):
        if phase == 0:
            spot, sem = self.index(k, 0, 0), self.sems[0].at[k]
        elif phase == 1:
            spot, sem = self.index(k, 0, j), self.sems[1].at[j, k]
        else:
            spot, sem = self.index(k, 1, j), self.sems[2].at[j, k]
        other = (self.me + 1) % self.count
        return remote(self.dst.at[spot], self.dst.at[spot], self.sent.at[phase, j, k], sem, other, self.subs)

    def relay(self, k):
        for j in range(1, self.subs):
            self.copy(1, j, k).start()
        if self.cores > 1:
            self.copy(2, 0, k).start()

    def start(self):
        self.dst[self.me] = self.src[...]

        @pl.loop(1, self.groups)
        def _(k):
            self.copy(0, 0, k).start()

        self.relay(0)

    def finish(self):
        @pl.loop(1, self.groups)
        def _(k):
            self.arrive(0, 0, k).wait_recv()
            self.relay(k)

        @pl.loop(0, self.groups)
        def _(k):
            for j in range(1, self.subs):
                self.arrive(1, j, k).wait_recv()
                if self.cores > 1:
                    self.copy(2, j, k).start()

        @pl.loop(0, self.groups)
        def _(k):
            for j in range(self.subs):
                if self.cores > 1:
                    self.arrive(2, j, k).wait_recv()
                    self.copy(2, j, k).wait_send()
                if j > 0:
                    self.copy(1, j, k).wait_send()

        @pl.loop(1, self.groups)
        def _(k):
            self.copy(0, 0, k).wait_send()


def spread_sems(count, subs):
    cores = 2 if count // subs % 2 == 0 else 1
    groups = count // subs // cores
    dma = pltpu.SemaphoreType.DMA
    return [dma((groups,)), dma((subs, groups)), dma((subs, groups)), dma((3, subs, groups))]


class Halo:
    def __init__(self, src, dst, sends, recvs, hops, sign):
        self.me, self.count, self.subs = place()
        self.src, self.dst, self.sends, self.recvs = src, dst, sends, recvs
        self.hops, self.sign = hops, sign
        self.paired = lax.axis_size("seq") % 2 == 0
        far_core = self.me // self.subs % 2
        self.first = far_core == (0 if sign > 0 else 1)

    def slot(self, d):
        return self.dst.at[self.hops - d if self.sign > 0 else d - 1]

    def inside(self, index):
        return (index >= 0) & (index < self.count)

    def cuts(self, d):
        if not self.paired or d <= self.subs:
            return self.inside(self.me + self.sign * d)
        target = self.me + self.sign * d + 2 * self.count * self.subs
        core = target // self.subs % 2
        return self.inside(self.me + self.sign * d) & (core == (0 if self.sign > 0 else 1))

    def direct(self, d):
        target = jnp.clip(self.me + self.sign * d, 0, self.count - 1)
        return remote(self.src, self.slot(d), self.sends.at[d - 1], self.recvs.at[d - 1], target, self.subs)

    def passed(self, d):
        target = jnp.clip(self.me + self.sign * self.subs, 0, self.count - 1)
        to = d + self.subs
        return remote(
            self.slot(d), self.slot(to), self.sends.at[self.hops + to - 1], self.recvs.at[to - 1],
            target, self.subs,
        )

    def relays(self, d):
        return self.first & self.inside(self.me - self.sign * d)

    def start(self):
        for d in range(1, self.hops + 1):
            @pl.when(self.cuts(d))
            def _():
                self.direct(d).start()

    def land(self, d):
        @pl.when(self.inside(self.me - self.sign * d))
        def _():
            self.direct(d).wait_recv()

        if self.paired and d + self.subs <= self.hops:
            @pl.when(self.relays(d))
            def _():
                self.passed(d).start()

    def finish(self):
        for d in range(1, self.hops + 1):
            self.land(d)

    def drain(self):
        for d in range(1, self.hops + 1):
            @pl.when(self.cuts(d))
            def _():
                self.direct(d).wait_send()

            if self.paired and d + self.subs <= self.hops:
                @pl.when(self.relays(d))
                def _():
                    self.passed(d).wait_send()


class Shift:
    def __init__(self, src, dst, send, recv, distance):
        me, count, subs = place()
        self.me, self.subs, self.target = me, subs, me + distance
        self.args = (src, dst, send, recv)
        self.sends = (me + distance >= 0) & (me + distance < count)
        self.gets = (me - distance >= 0) & (me - distance < count)
        self.copy = remote(src, dst, send, recv, jnp.clip(me + distance, 0, count - 1), subs)

    def start(self):
        @pl.when(self.sends)
        def _():
            self.copy.start()

    def wait(self):
        @pl.when(self.sends)
        def _():
            self.copy.wait_send()

        @pl.when(self.gets)
        def _():
            self.copy.wait_recv()


def window_masks(hops, rows, me):
    margin = hops * rows
    row = iota((2 * rows, rows), 0) % rows
    masks = []
    for b in range(hops + 1):
        least, most = margin - (b + 1) * rows + 1, margin + rows - 1 - b * rows
        gap = margin - b * rows + row - iota((2 * rows, rows), 1)
        mask = jnp.broadcast_to(me - (hops - b), gap.shape) >= 0
        if least < 0:
            mask = mask & (gap >= 0)
        if most >= WINDOW:
            mask = mask & (gap < WINDOW)
        masks.append(mask)
    return masks


def causal(keys, queries):
    return keys <= queries


class Coarse:
    def __init__(self, total, span, base, cw, cow, scratch):
        self.total, self.span, self.base = total, span, base
        self.cw, self.cow = cw, cow
        self.uq, self.fq, self.uk, self.fk, self.v, self.g = scratch
        self.width = cw.shape[2]

    def grads(self, cg):
        self.gb = dot_nt(cg, self.cow[...]).astype(BF16)
        self.g[pl.ds(0, self.total), :] = self.gb.astype(F32)

    def project(self, normed):
        uq, fq = head_rms(dot(normed, self.cw[0]))
        uk, fk = head_rms(dot(normed, self.cw[1]))
        v = dot(normed, self.cw[2])
        for ref, value in ((self.uq, uq), (self.fq, fq), (self.uk, uk), (self.fk, fk), (self.v, v)):
            ref[pl.ds(0, self.total), :] = value
        self.qb, self.kb, self.vb = (uq * QUERY).astype(BF16), uk.astype(BF16), v.astype(BF16)

    def sums(self, cols):
        block = min(self.total, 256)
        inverse, deltas = [], []
        for i in range(self.total // block):
            part = slice(i * block, (i + 1) * block)
            q, g = self.qb[part, cols], self.gb[part, cols]
            t, d = [0.0, 0.0], [0.0, 0.0]
            for j in range(i + 1):
                rows = slice(j * block, (j + 1) * block)
                e = jnp.exp2(dot_nt(both(self.kb[rows, cols]), q))
                if j == i:
                    e = jnp.where(causal(iota(e.shape, 0) % block, iota(e.shape, 1)), e, 0.0)
                ed = e * dot_nt(both(self.vb[rows, cols]), g)
                for h in range(2):
                    half = slice(h * block, (h + 1) * block)
                    t[h] = t[h] + jnp.sum(e[half], axis=0, keepdims=True)
                    d[h] = d[h] + jnp.sum(ed[half], axis=0, keepdims=True)
            inverse.append([1.0 / x for x in t])
            deltas.append([x * r for x, r in zip(d, inverse[-1])])
        join = lambda parts, h: jnp.concatenate([x[h] for x in parts], axis=1)
        return [join(inverse, h) for h in range(2)], [join(deltas, h) for h in range(2)]

    def mine(self, ref, cols):
        start = pl.multiple_of(self.base, 8)
        return ref[pl.ds(start, self.span), cols]

    def attend(self):
        span, total = self.span, self.total
        shape = (2 * span, total)
        own = self.base + iota(shape, 0) % span
        after = causal(own, iota(shape, 1))
        before = causal(iota(shape, 1), own)
        att_p, dq_p, dk_p, dv_p = [], [], [], []
        for p in range(self.width // PAIR):
            cols = slice(p * PAIR, (p + 1) * PAIR)
            inverse, deltas = self.sums(cols)
            ds_cols = pl.ds(p * PAIR, PAIR)
            qp, kp, vp, gp = self.qb[:, cols], self.kb[:, cols], self.vb[:, cols], self.gb[:, cols]
            k2, v2 = both(self.mine(self.uk, ds_cols)), both(self.mine(self.v, ds_cols))
            q2, g2 = both(self.mine(self.uq, ds_cols) * QUERY), both(self.mine(self.g, ds_cols))
            wide = lambda pair: jnp.concatenate([jnp.broadcast_to(x, (span, total)) for x in pair])
            pt = jnp.where(after, jnp.exp2(dot_nt(k2, qp)) * wide(inverse), 0.0)
            dst = pt * (dot_nt(v2, gp) - wide(deltas))
            dk_p.append(pick(dot(dst.astype(BF16), qp)) * LN2)
            dv_p.append(pick(dot(pt.astype(BF16), gp)))
            e = jnp.where(before, jnp.exp2(dot_nt(q2, kp)), 0.0)
            e = e * (1.0 / jnp.sum(e, axis=-1, keepdims=True))
            dp = dot_nt(g2, vp)
            delta = jnp.sum(e * dp, axis=-1, keepdims=True)
            ds = e * (dp - delta)
            dq_p.append(pick(dot(ds.astype(BF16), kp)) * SCALE)
            att_p.append(pick(dot(e.astype(BF16), vp)))
        join = lambda parts: jnp.concatenate(parts, axis=1)
        return join(att_p), join(dq_p), join(dk_p), join(dv_p)

    def finish(self, outs_all):
        every = pl.ds(0, self.width)
        att, dq, dk, dv = self.attend()
        mixed = dot(att[:outs_all].astype(BF16), self.cow[...])
        dq = head_back(dq, self.mine(self.uq, every), self.mine(self.fq, every)).astype(BF16)
        dk = head_back(dk, self.mine(self.uk, every), self.mine(self.fk, every)).astype(BF16)
        dv = dv.astype(BF16)
        return mixed, dot_nt(dq, self.cw[0]) + dot_nt(dk, self.cw[1]) + dot_nt(dv, self.cw[2])


def layer_pair(
    hops, x_ref, cot_ref, w_hbm, out_hbm, cw_hbm, cow_hbm, output_ref, grad_ref,
    w_ref, out_w, cw, cow, before, q_all, cot_after, k_all, v_all,
    unit_q, unit_k, scale_q, scale_k, e_ref, t_ref, acc_ref, rt_ref, att_ref, hidden_ref,
    cg_own, cg_all, pool_own, pool_all, pooled, gcot, g_all,
    uq2, fq2, uk2, fk2, v2, g2, mixed_ref, ng_ref, x_out, x_in, stats, stats_after, dq_ref,
    load, halo_sends, halo_recvs, x_sems, stat_sems, *sems,
):
    me, count, subs = place()
    mine, seq = lax.axis_index("sub"), lax.axis_index("seq")
    rows = x_ref.shape[0]
    outs = rows // POOL
    margin, length = hops * rows, (hops + 1) * rows
    total = count * outs
    far = (hops + 2) * outs
    greet_all()
    parts = [
        (w_hbm.at[1], w_ref.at[1]), (w_hbm.at[2], w_ref.at[2]), (w_hbm.at[0], w_ref.at[0]),
        (out_hbm, out_w), (cw_hbm, cw), (cow_hbm, cow),
    ]
    loads = [pltpu.make_async_copy(src, dst, load.at[i]) for i, (src, dst) in enumerate(parts)]
    for one in loads:
        one.start()
    for d in range(1, hops + 1):
        @pl.when(me - d < 0)
        def _():
            before[hops - d] = jnp.zeros((rows, D), BF16)

        @pl.when(me + d >= count)
        def _():
            q_all[d] = jnp.zeros((rows, D), BF16)
            cot_after[d - 1] = jnp.zeros((rows, D), BF16)
            stats_after[d - 1] = jnp.zeros(stats.shape, F32)

    extra = pooled.shape[0] - total
    pooled[pl.ds(total, extra), :] = jnp.zeros((extra, D), F32)
    cg_all[pl.ds(count, extra // outs)] = jnp.zeros((extra // outs, outs, D), BF16)
    for ref in (uq2, fq2, uk2, fk2, v2, g2):
        ref[pl.ds(total, extra), :] = jnp.zeros((extra, ref.shape[1]), F32)
    groups = (iota((outs, rows), 1) // POOL == iota((outs, rows), 0)).astype(F32).astype(BF16)
    cg_own[...] = dot(groups, cot_ref[...]).astype(BF16)
    own = x_ref[...].astype(F32)
    own_b = rms_rows(own)[0].astype(BF16)
    down = Halo(x_ref, before, halo_sends.at[0], halo_recvs.at[0], hops, 1)
    up_cot = Halo(cot_ref, cot_after, halo_sends.at[1], halo_recvs.at[1], hops, -1)
    up = Halo(q_all.at[0], q_all.at[pl.ds(1, hops)], halo_sends.at[2], halo_recvs.at[2], hops, -1)
    cg_spread = Spread(cg_own, cg_all, *sems[:4])
    pool_spread = Spread(pool_own, pool_all, *sems[4:])
    met_all()
    down.start()
    cg_spread.start()
    up_cot.start()
    loads[0].wait()
    unit, factor = head_rms(dot(own_b, w_ref[1]))
    k_all[pl.ds(margin, rows), :] = unit.astype(BF16)
    unit_k[...] = unit
    scale_k[...] = factor
    loads[1].wait()
    v_all[pl.ds(margin, rows), :] = dot(own_b, w_ref[2]).astype(BF16)
    loads[2].wait()
    unit, factor = head_rms(dot(own_b, w_ref[0]))
    q_all[0] = (unit * QUERY).astype(BF16)
    unit_q[...] = unit
    scale_q[...] = factor
    cg_spread.finish()

    def keys(d):
        slot = pl.ds(margin - d * rows, rows)
        prev = rms_rows(before[hops - d].astype(F32))[0].astype(BF16)
        k_all[slot, :] = head_rms(dot(prev, w_ref[1]))[0].astype(BF16)
        v_all[slot, :] = dot(prev, w_ref[2]).astype(BF16)

    masks = window_masks(hops, rows, me)

    def scores(p, low, high):
        cols = pl.ds(p * PAIR, PAIR)
        span = pl.ds(low * rows, (high - low) * rows)
        s = dot_nt(both(q_all[0, :, cols]), k_all[span, cols])
        e = [
            jnp.where(masks[b], jnp.exp2(s[:, (b - low) * rows : (b - low + 1) * rows]), 0.0)
            for b in range(low, high)
        ]
        e_b = jnp.concatenate(e, axis=1).astype(BF16)
        e_ref[p, :, span] = e_b
        return functools.reduce(jnp.add, e), dot(e_b, v_all[span, cols])

    half = hops // 2
    for d in range(1, hops - half + 1):
        down.land(d)
        keys(d)
    for p in range(HEADS // 2):
        t_ref[p], acc_ref[p] = scores(p, half, hops + 1)
    for d in range(hops - half + 1, hops + 1):
        down.land(d)
        keys(d)
    lane = iota((rows, 128), 1)
    totals = jnp.ones((rows, 128), F32)
    for p in range(HEADS // 2):
        t, acc = scores(p, 0, half)
        t = jnp.sum(t + t_ref[p], axis=-1, keepdims=True)
        inverse = jnp.broadcast_to(1.0 / t, (2 * rows, PAIR))
        rt_ref[p] = inverse
        att_ref[:, pl.ds(p * PAIR, PAIR)] = pick((acc + acc_ref[p]) * inverse).astype(BF16)
        totals = jnp.where(lane == 2 * p, t[:rows], totals)
        totals = jnp.where(lane == 2 * p + 1, t[rows:], totals)
    loads[3].wait()
    hidden = (own + dot(att_ref[...], out_w[...])).astype(BF16)
    hidden_ref[...] = hidden
    back = iota((outs, rows), 0) * POOL - iota((outs, rows), 1)
    part = dot(((back >= 0) & (back < POOL)).astype(F32).astype(BF16), hidden)
    tail = dot((iota((outs, rows), 1) > rows - POOL).astype(F32).astype(BF16), hidden)
    lanes = D // outs
    folded = jnp.zeros((outs, lanes), F32)
    for c in range(outs):
        folded = jnp.where(iota((outs, lanes), 0) == c, tail[:, c * lanes : (c + 1) * lanes], folded)
    pool_own[...] = (jnp.concatenate([part, folded], axis=1) / POOL).astype(BF16)
    pool_spread.start()
    up.start()
    up_cot.finish()
    loads[4].wait()
    loads[5].wait()
    base = seq * subs * outs
    span = (subs - 1) * outs + far
    coarse = Coarse(total, span, base, cw, cow, (uq2, fq2, uk2, fk2, v2, g2))
    coarse.grads(cg_all[pl.ds(0, count)].astype(F32).reshape(total, D).astype(BF16))
    gcot[pl.ds(0, rows), :] = dot_nt(cot_ref[...], out_w[...])
    gcot[pl.ds(rows, margin), :] = dot_nt(cot_after[...].reshape(margin, D), out_w[...])
    stats[pl.ds(0, HEADS), :] = jnp.log2(totals.T[:HEADS])
    pool_spread.finish()
    got = pool_all[...].astype(F32).reshape(total, D + lanes)
    block = min(total, 256)
    place_at = (iota((block, block), 0) // outs == iota((block, block), 1) // outs) & (iota((block, block), 0) % outs == 0)
    place_at = place_at.astype(F32).astype(BF16)
    tails = []
    for i in range(total // block):
        one = got[i * block : (i + 1) * block, D:]
        wide = [jnp.where(iota(one.shape, 0) % outs == c, one, 0.0) for c in range(outs)]
        tails.append(dot(place_at, jnp.concatenate(wide, axis=1).astype(BF16)))
    tails = jnp.concatenate([jnp.zeros((outs, D), F32)] + tails)[:total]
    pooled_v = (got[:, :D] + tails).astype(BF16).astype(F32)
    pooled[pl.ds(0, total), :] = pooled_v
    coarse.project(rms_rows(pooled_v)[0].astype(BF16))
    mixed, ng = coarse.finish(subs * outs)
    mixed_ref[...] = mixed
    ng_ref[...] = ng

    def cut(sub):
        start = pl.multiple_of(sub * outs, outs)
        return mixed_ref[pl.ds(start, outs), :], ng_ref[pl.ds(start, far), :]

    copies = []
    for k in range(1, subs):
        other = (mine + k) % subs
        x_out[k] = jnp.concatenate(cut(other)).astype(BF16)
        copies.append(remote(
            x_out.at[k], x_in.at[k], x_sems.at[0, k], x_sems.at[1, k], seq * subs + other, subs
        ))
        copies[-1].start()
    mixed, ng = cut(mine)
    start = pl.multiple_of(me * outs, outs)
    pooled_own = pooled[pl.ds(start, far), :]
    cg = cg_all[pl.ds(me, far // outs)].astype(F32).reshape(far, D)
    normed, factor = rms_rows(pooled_own)
    for copy in copies:
        copy.wait()
    for k in range(1, subs):
        other = x_in[k].astype(F32)
        mixed, ng = mixed + other[:outs], ng + other[outs:]
    pg = (cg + row_back(ng, normed, factor)) / POOL
    pg = jnp.where(me * outs + iota(pg.shape, 0) < total, pg, 0.0).astype(BF16)
    pgw = dot_nt(pg, out_w[...]).astype(BF16)
    lift = ((iota((length, far), 0) + POOL - 1) // POOL == iota((length, far), 1)).astype(F32).astype(BF16)
    g_all[...] = (gcot[...] + dot(lift, pgw)).astype(BF16)
    delta = head_sum(g_all[pl.ds(0, rows), :].astype(F32) * att_ref[...].astype(F32))
    stats[pl.ds(HEADS, HEADS), :] = delta.T[:HEADS]
    moves = [
        Shift(stats, stats_after.at[d - 1], stat_sems.at[0, d - 1], stat_sems.at[1, d - 1], -d)
        for d in range(1, hops + 1)
    ]
    for move in moves:
        move.start()
    up.finish()
    state = (pooled_own[:outs] + mixed).astype(BF16)
    onto = (iota((rows, outs), 0) // POOL == iota((rows, outs), 1)).astype(F32).astype(BF16)
    output_ref[...] = (hidden_ref[...].astype(F32) + dot(onto, state)).astype(BF16)
    for p in range(HEADS // 2):
        cols = pl.ds(p * PAIR, PAIR)
        dp = dot_nt(both(g_all[pl.ds(0, rows), cols]), v_all[:, cols])
        column = jnp.concatenate([delta[:, 2 * p : 2 * p + 1], delta[:, 2 * p + 1 : 2 * p + 2]])
        ds = (e_ref[p].astype(F32) * (dp - column)).astype(BF16)
        dq_ref[:, cols] = pick(dot(ds, k_all[:, cols]) * rt_ref[p]) * SCALE
    for move in moves:
        move.wait()
    gap = iota((rows, length), 1) - iota((rows, length), 0)
    mask_t = (gap >= 0) & (gap < WINDOW)
    every = jnp.concatenate([stats[...]] + [stats_after[d] for d in range(hops)], axis=1)
    dk_p, dv_p = [], []
    for p in range(HEADS // 2):
        cols = pl.ds(p * PAIR, PAIR)
        own_slot = pl.ds(margin, rows)
        qp, gp = q_all[:, :, cols].reshape(length, PAIR), g_all[:, cols]
        st = dot_nt(both(k_all[own_slot, cols]), qp)
        dpt = dot_nt(both(v_all[own_slot, cols]), gp)
        pts, dsts = [], []
        for h in range(2):
            head = 2 * p + h
            part = slice(h * rows, (h + 1) * rows)
            pt = jnp.where(mask_t, jnp.exp2(st[part] - every[head : head + 1]), 0.0)
            pts.append(pt.astype(BF16))
            dsts.append((pt * (dpt[part] - every[HEADS + head : HEADS + head + 1])).astype(BF16))
        dk_p.append(pick(dot(jnp.concatenate(dsts), qp)) * LN2)
        dv_p.append(pick(dot(jnp.concatenate(pts), gp)))
    join = lambda parts: jnp.concatenate(parts, axis=1)
    dq = head_back(dq_ref[...], unit_q[...], scale_q[...]).astype(BF16)
    dk = head_back(join(dk_p), unit_k[...], scale_k[...]).astype(BF16)
    dv = join(dv_p).astype(BF16)
    grads = dot_nt(dq, w_ref[0]) + dot_nt(dk, w_ref[1]) + dot_nt(dv, w_ref[2])
    normed, factor = rms_rows(x_ref[...].astype(F32))
    hidden_grad = cot_ref[...].astype(F32) + dot(lift[:rows], pg)
    grad_ref[...] = (hidden_grad + row_back(grads, normed, factor)).astype(BF16)
    down.drain()
    up_cot.drain()
    up.drain()


def per_device(tokens, cotangent, fine_qkv, fine_out, coarse_qkv, coarse_out):
    rows = tokens.shape[0]
    hops = -(-WINDOW // rows)
    outs = rows // POOL
    me, count, subs = place()
    far = (hops + 2) * outs
    length = (hops + 1) * rows
    total = count * outs
    span = (subs - 1) * outs + far
    width = coarse_qkv.shape[2]
    pairs = HEADS // 2
    shape = jax.ShapeDtypeStruct
    dma = pltpu.SemaphoreType.DMA
    vmem = pltpu.VMEM
    fine_w = jnp.transpose(fine_qkv, (1, 0, 2))
    coarse_w = jnp.transpose(coarse_qkv, (1, 0, 2))
    wide = D + D // outs
    padded = total + far
    scratch = [
        vmem(fine_w.shape, BF16), vmem(fine_out.shape, BF16), vmem(coarse_w.shape, BF16),
        vmem(coarse_out.shape, BF16),
        vmem((hops, rows, D), BF16), vmem((hops + 1, rows, D), BF16), vmem((hops, rows, D), BF16),
        vmem((length, D), BF16), vmem((length, D), BF16),
        vmem((rows, D), F32), vmem((rows, D), F32), vmem((rows, D), F32), vmem((rows, D), F32),
        vmem((pairs, 2 * rows, length), BF16), vmem((pairs, 2 * rows, rows), F32),
        vmem((pairs, 2 * rows, PAIR), F32), vmem((pairs, 2 * rows, PAIR), F32),
        vmem((rows, D), BF16), vmem((rows, D), BF16),
        vmem((outs, D), BF16), vmem((count + far // outs, outs, D), BF16),
        vmem((outs, wide), BF16), vmem((count, outs, wide), BF16),
        vmem((padded, D), F32), vmem((length, D), F32), vmem((length, D), BF16),
    ] + [vmem((padded, width), F32)] * 6 + [
        vmem((subs * outs, D), F32), vmem((span, D), F32),
        vmem((subs, outs + far, D), BF16), vmem((subs, outs + far, D), BF16),
        vmem((2 * HEADS, rows), F32), vmem((hops, 2 * HEADS, rows), F32), vmem((rows, D), F32),
        dma((6,)), dma((3, 2 * hops)), dma((3, hops)), dma((2, subs)), dma((2, hops)),
    ] + spread_sems(count, subs) * 2
    return pl.pallas_call(
        functools.partial(layer_pair, hops),
        out_shape=[shape((rows, D), BF16)] * 2,
        in_specs=[VMEM] * 2 + [ANY] * 4,
        out_specs=[VMEM] * 2,
        scratch_shapes=scratch,
        compiler_params=pltpu.CompilerParams(
            collective_id=0, has_side_effects=True, vmem_limit_bytes=67043328
        ),
    )(tokens, cotangent, fine_w, fine_out, coarse_w, coarse_out)


def solution(mesh):
    placed = (
        P(("seq", "sub"), None),
        P(("seq", "sub"), None),
        P(),
        P(),
        P(None, None, "sub"),
        P("sub", None),
    )
    return jax.shard_map(
        per_device,
        mesh=mesh,
        in_specs=placed,
        out_specs=(P(("seq", "sub"), None), P(("seq", "sub"), None)),
        check_vma=False,
    )
```

```python
import functools
import math

import jax
import jax.numpy as jnp
from jax import lax
from jax.experimental import pallas as pl
from jax.experimental.pallas import tpu as pltpu
from jax.sharding import PartitionSpec as P

D = 1024
HEADS = 16
HEAD_DIM = 64
WINDOW = 512
POOL = 16
EPS = 1e-06
F32 = jnp.float32
BF16 = jnp.bfloat16
MESH = pl.DeviceIdType.MESH
PAIR = 2 * HEAD_DIM
SCALE = HEAD_DIM ** (-0.5)
LN2 = math.log(2.0)
QUERY = SCALE / LN2
VMEM = pl.BlockSpec(memory_space=pltpu.VMEM)
HBM = pl.BlockSpec(memory_space=pltpu.HBM)
SMEM = pl.BlockSpec(memory_space=pltpu.SMEM)


def dot(a, b):
    return jnp.dot(a, b, preferred_element_type=F32)


def dot_nt(a, b):
    return lax.dot_general(a, b, (((1,), (1,)), ((), ())), preferred_element_type=F32)


def dot_tn(a, b):
    return lax.dot_general(a, b, (((0,), (0,)), ((), ())), preferred_element_type=F32)


def split(x):
    hi = x.astype(BF16)
    return hi, (x - hi.astype(F32)).astype(BF16)


def iota(shape, axis):
    return lax.broadcasted_iota(jnp.int32, shape, axis)


def head_sum(x):
    group = (iota((x.shape[1], 128), 0) // HEAD_DIM == iota((x.shape[1], 128), 1)).astype(F32).astype(BF16)
    hi, lo = split(x)
    return dot(hi, group) + dot(lo, group)


def head_mean(x):
    group = iota((PAIR, PAIR), 0) // HEAD_DIM == iota((PAIR, PAIR), 1) // HEAD_DIM
    group = jnp.where(group, 1.0 / HEAD_DIM, 0.0).astype(BF16)
    x = x.astype(BF16)
    return jnp.concatenate([dot(x[:, c : c + PAIR], group) for c in range(0, x.shape[1], PAIR)], axis=1)


def head_rms(raw):
    factor = lax.rsqrt(head_mean(raw * raw) + EPS)
    return raw * factor, factor


def head_back(grad, unit, factor):
    return factor * (grad - unit * head_mean(unit * grad))


def rms_rows(x):
    factor = lax.rsqrt(jnp.mean(x * x, axis=-1, keepdims=True) + EPS)
    return x * factor, factor


def row_back(grad, normed, factor):
    return factor * (grad - normed * jnp.mean(normed * grad, axis=-1, keepdims=True))


def both(pair):
    low = iota(pair.shape, 1) < HEAD_DIM
    wide = pair.astype(F32)
    return jnp.concatenate([jnp.where(low, wide, 0.0), jnp.where(low, 0.0, wide)]).astype(BF16)


def pick(stacked):
    half = stacked.shape[0] // 2
    low = iota((half, PAIR), 1) < HEAD_DIM
    return jnp.where(low, stacked[:half], stacked[half:])


def place():
    subs = lax.axis_size("sub")
    count = lax.axis_size("seq") * subs
    me = lax.axis_index("seq") * subs + lax.axis_index("sub")
    return me, count, subs


def coords(index, subs):
    return (index // subs, index % subs)


def greet_all():
    me, count, subs = place()
    barrier = pltpu.get_barrier_semaphore()

    @pl.loop(1, count)
    def _(k):
        pl.semaphore_signal(
            barrier, inc=1, device_id=coords((me + k) % count, subs), device_id_type=MESH
        )


def met_all():
    pl.semaphore_wait(pltpu.get_barrier_semaphore(), lax.axis_size("seq") * lax.axis_size("sub") - 1)


def remote(src, dst, send, recv, target, subs):
    return pltpu.make_async_remote_copy(
        src_ref=src, dst_ref=dst, send_sem=send, recv_sem=recv,
        device_id=coords(target, subs), device_id_type=MESH,
    )


class Spread:
    def __init__(self, src, dst, out_sem, mid_sem, last_sem, sent):
        self.me, self.count, self.subs = place()
        self.cores = 2 if lax.axis_size("seq") % 2 == 0 else 1
        self.groups = self.count // self.subs // self.cores
        self.sub = self.me % self.subs
        self.core = self.me // self.subs % self.cores
        self.group = self.me // self.subs // self.cores
        self.src, self.dst, self.sems, self.sent = src, dst, (out_sem, mid_sem, last_sem), sent

    def index(self, k, core, j):
        group = (self.group + self.groups - k) % self.groups
        sub = (self.sub + self.subs - j) % self.subs
        return (group * self.cores + (self.core + core) % self.cores) * self.subs + sub

    def copy(self, phase, j, k):
        if phase == 0:
            spot, source = self.me, self.src
            target, sem = self.index(self.groups - k, 0, 0), self.sems[0].at[k]
        elif phase == 1:
            spot = self.index(k, 0, 0)
            target, sem = self.index(0, 0, self.subs - j), self.sems[1].at[j, k]
        else:
            spot = self.index(k, 0, j)
            target, sem = self.index(0, 1, 0), self.sems[2].at[j, k]
        source = self.src if phase == 0 else self.dst.at[spot]
        return remote(source, self.dst.at[spot], self.sent.at[phase, j, k], sem, target, self.subs)

    def arrive(self, phase, j, k):
        if phase == 0:
            spot, sem = self.index(k, 0, 0), self.sems[0].at[k]
        elif phase == 1:
            spot, sem = self.index(k, 0, j), self.sems[1].at[j, k]
        else:
            spot, sem = self.index(k, 1, j), self.sems[2].at[j, k]
        other = (self.me + 1) % self.count
        return remote(self.dst.at[spot], self.dst.at[spot], self.sent.at[phase, j, k], sem, other, self.subs)

    def relay(self, k):
        for j in range(1, self.subs):
            self.copy(1, j, k).start()
        if self.cores > 1:
            self.copy(2, 0, k).start()

    def start(self):
        self.dst[self.me] = self.src[...]

        @pl.loop(1, self.groups)
        def _(k):
            self.copy(0, 0, k).start()

        self.relay(0)

    def widen(self):
        @pl.loop(1, self.groups)
        def _(k):
            self.arrive(0, 0, k).wait_recv()
            self.relay(k)

    def cross(self):
        @pl.loop(0, self.groups)
        def _(k):
            for j in range(1, self.subs):
                self.arrive(1, j, k).wait_recv()
                if self.cores > 1:
                    self.copy(2, j, k).start()

    def finish(self):
        @pl.loop(0, self.groups)
        def _(k):
            for j in range(self.subs):
                if self.cores > 1:
                    self.arrive(2, j, k).wait_recv()
                    self.copy(2, j, k).wait_send()
                if j > 0:
                    self.copy(1, j, k).wait_send()

        @pl.loop(1, self.groups)
        def _(k):
            self.copy(0, 0, k).wait_send()


def spread_sems(count, subs):
    cores = 2 if count // subs % 2 == 0 else 1
    groups = count // subs // cores
    dma = pltpu.SemaphoreType.DMA
    return [dma((groups,)), dma((subs, groups)), dma((subs, groups)), dma((3, subs, groups))]


class Halo:
    def __init__(self, src, dst, sends, recvs, hops, sign):
        self.me, self.count, self.subs = place()
        self.src, self.dst, self.sends, self.recvs = src, dst, sends, recvs
        self.hops, self.sign = hops, sign
        self.paired = lax.axis_size("seq") % 2 == 0
        far_core = self.me // self.subs % 2
        self.first = far_core == (0 if sign > 0 else 1)

    def slot(self, d):
        return self.dst.at[self.hops - d if self.sign > 0 else d - 1]

    def inside(self, index):
        return (index >= 0) & (index < self.count)

    def cuts(self, d):
        if not self.paired or d <= self.subs:
            return self.inside(self.me + self.sign * d)
        target = self.me + self.sign * d + 2 * self.count * self.subs
        core = target // self.subs % 2
        return self.inside(self.me + self.sign * d) & (core == (0 if self.sign > 0 else 1))

    def direct(self, d):
        target = jnp.clip(self.me + self.sign * d, 0, self.count - 1)
        return remote(self.src, self.slot(d), self.sends.at[d - 1], self.recvs.at[d - 1], target, self.subs)

    def passed(self, d):
        target = jnp.clip(self.me + self.sign * self.subs, 0, self.count - 1)
        to = d + self.subs
        return remote(
            self.slot(d), self.slot(to), self.sends.at[self.hops + to - 1], self.recvs.at[to - 1],
            target, self.subs,
        )

    def relays(self, d):
        return self.first & self.inside(self.me - self.sign * d)

    def start(self):
        for d in range(1, self.hops + 1):
            @pl.when(self.cuts(d))
            def _():
                self.direct(d).start()

    def land(self, d):
        @pl.when(self.inside(self.me - self.sign * d))
        def _():
            self.direct(d).wait_recv()

        if self.paired and d + self.subs <= self.hops:
            @pl.when(self.relays(d))
            def _():
                self.passed(d).start()

    def finish(self):
        for d in range(1, self.hops + 1):
            self.land(d)

    def drain(self):
        for d in range(1, self.hops + 1):
            @pl.when(self.cuts(d))
            def _():
                self.direct(d).wait_send()

            if self.paired and d + self.subs <= self.hops:
                @pl.when(self.relays(d))
                def _():
                    self.passed(d).wait_send()


class Shift:
    def __init__(self, src, dst, send, recv, distance):
        me, count, subs = place()
        self.me, self.subs, self.target = me, subs, me + distance
        self.args = (src, dst, send, recv)
        self.sends = (me + distance >= 0) & (me + distance < count)
        self.gets = (me - distance >= 0) & (me - distance < count)
        self.copy = remote(src, dst, send, recv, jnp.clip(me + distance, 0, count - 1), subs)

    def start(self):
        @pl.when(self.sends)
        def _():
            self.copy.start()

    def wait(self):
        @pl.when(self.sends)
        def _():
            self.copy.wait_send()

        @pl.when(self.gets)
        def _():
            self.copy.wait_recv()


def window_masks(hops, rows, me):
    margin = hops * rows
    row = iota((2 * rows, rows), 0) % rows
    masks = []
    for b in range(hops + 1):
        least, most = margin - (b + 1) * rows + 1, margin + rows - 1 - b * rows
        gap = margin - b * rows + row - iota((2 * rows, rows), 1)
        mask = jnp.broadcast_to(me - (hops - b), gap.shape) >= 0
        if least < 0:
            mask = mask & (gap >= 0)
        if most >= WINDOW:
            mask = mask & (gap < WINDOW)
        masks.append(mask)
    return masks


def causal(keys, queries):
    return keys <= queries


class Coarse:
    def __init__(self, total, span, base, cw, cow, scratch):
        self.total, self.span, self.base = total, span, base
        self.cw, self.cow = cw, cow
        self.uq, self.fq, self.uk, self.fk, self.v, self.g = scratch
        self.width = cw.shape[2]

    def grads(self, cg):
        self.gb = dot_nt(cg, self.cow[...]).astype(BF16)
        self.g[pl.ds(0, self.total), :] = self.gb.astype(F32)

    def project(self, normed):
        uq, fq = head_rms(dot(normed, self.cw[0]))
        uk, fk = head_rms(dot(normed, self.cw[1]))
        v = dot(normed, self.cw[2])
        for ref, value in ((self.uq, uq), (self.fq, fq), (self.uk, uk), (self.fk, fk), (self.v, v)):
            ref[pl.ds(0, self.total), :] = value
        self.qb, self.kb, self.vb = (uq * QUERY).astype(BF16), uk.astype(BF16), v.astype(BF16)

    def sums(self, cols):
        block = min(self.total, 256)
        inverse, deltas = [], []
        for i in range(self.total // block):
            part = slice(i * block, (i + 1) * block)
            q, g = self.qb[part, cols], self.gb[part, cols]
            t, d = [0.0, 0.0], [0.0, 0.0]
            for j in range(i + 1):
                rows = slice(j * block, (j + 1) * block)
                e = jnp.exp2(dot_nt(both(self.kb[rows, cols]), q))
                if j == i:
                    e = jnp.where(causal(iota(e.shape, 0) % block, iota(e.shape, 1)), e, 0.0)
                ed = e * dot_nt(both(self.vb[rows, cols]), g)
                for h in range(2):
                    half = slice(h * block, (h + 1) * block)
                    t[h] = t[h] + jnp.sum(e[half], axis=0, keepdims=True)
                    d[h] = d[h] + jnp.sum(ed[half], axis=0, keepdims=True)
            inverse.append([1.0 / x for x in t])
            deltas.append([x * r for x, r in zip(d, inverse[-1])])
        join = lambda parts, h: jnp.concatenate([x[h] for x in parts], axis=1)
        return [join(inverse, h) for h in range(2)], [join(deltas, h) for h in range(2)]

    def mine(self, ref, cols):
        start = pl.multiple_of(self.base, 8)
        return ref[pl.ds(start, self.span), cols]

    def attend(self):
        span, total = self.span, self.total
        shape = (2 * span, total)
        own = self.base + iota(shape, 0) % span
        after = causal(own, iota(shape, 1))
        before = causal(iota(shape, 1), own)
        att_p, dq_p, dk_p, dv_p = [], [], [], []
        for p in range(self.width // PAIR):
            cols = slice(p * PAIR, (p + 1) * PAIR)
            inverse, deltas = self.sums(cols)
            ds_cols = pl.ds(p * PAIR, PAIR)
            qp, kp, vp, gp = self.qb[:, cols], self.kb[:, cols], self.vb[:, cols], self.gb[:, cols]
            k2, v2 = both(self.mine(self.uk, ds_cols)), both(self.mine(self.v, ds_cols))
            q2, g2 = both(self.mine(self.uq, ds_cols) * QUERY), both(self.mine(self.g, ds_cols))
            wide = lambda pair: jnp.concatenate([jnp.broadcast_to(x, (span, total)) for x in pair])
            pt = jnp.where(after, jnp.exp2(dot_nt(k2, qp)) * wide(inverse), 0.0)
            dst = pt * (dot_nt(v2, gp) - wide(deltas))
            dk_p.append(pick(dot(dst.astype(BF16), qp)) * LN2)
            dv_p.append(pick(dot(pt.astype(BF16), gp)))
            e = jnp.where(before, jnp.exp2(dot_nt(q2, kp)), 0.0)
            e = e * (1.0 / jnp.sum(e, axis=-1, keepdims=True))
            dp = dot_nt(g2, vp)
            delta = jnp.sum(e * dp, axis=-1, keepdims=True)
            ds = e * (dp - delta)
            dq_p.append(pick(dot(ds.astype(BF16), kp)) * SCALE)
            att_p.append(pick(dot(e.astype(BF16), vp)))
        join = lambda parts: jnp.concatenate(parts, axis=1)
        return join(att_p), join(dq_p), join(dk_p), join(dv_p)

    def finish(self, outs_all):
        every = pl.ds(0, self.width)
        att, dq, dk, dv = self.attend()
        mixed = dot(att[:outs_all].astype(BF16), self.cow[...])
        dq = head_back(dq, self.mine(self.uq, every), self.mine(self.fq, every)).astype(BF16)
        dk = head_back(dk, self.mine(self.uk, every), self.mine(self.fk, every)).astype(BF16)
        dv = dv.astype(BF16)
        return mixed, dot_nt(dq, self.cw[0]) + dot_nt(dk, self.cw[1]) + dot_nt(dv, self.cw[2])


def layer_pair(
    hops, x_hbm, cot_hbm, w_hbm, out_hbm, cw_hbm, cow_hbm, output_ref, grad_ref,
    x_ref, cot_ref,
    w_ref, out_w, cw, cow, before, q_all, cot_after, k_all, v_all,
    unit_q, unit_k, scale_q, scale_k, e_ref, t_ref, acc_ref, rt_ref, att_ref, hidden_ref,
    cg_own, cg_all, pool_own, pool_all, pooled, gcot, g_all,
    uq2, fq2, uk2, fk2, v2, g2, mixed_ref, ng_ref, x_out, x_in, stats, stats_after, dq_ref,
    load, halo_sends, halo_recvs, x_sems, stat_sems, *sems,
):
    me, count, subs = place()
    mine, seq = lax.axis_index("sub"), lax.axis_index("seq")
    rows = x_ref.shape[0]
    outs = rows // POOL
    margin, length = hops * rows, (hops + 1) * rows
    total = count * outs
    far = (hops + 2) * outs
    greet_all()
    parts = [
        (w_hbm.at[1], w_ref.at[1]), (w_hbm.at[2], w_ref.at[2]), (w_hbm.at[0], w_ref.at[0]),
        (out_hbm, out_w), (cw_hbm, cw), (cow_hbm, cow), (x_hbm, x_ref), (cot_hbm, cot_ref),
    ]
    loads = [pltpu.make_async_copy(src, dst, load.at[i]) for i, (src, dst) in enumerate(parts)]
    for one in loads[6:] + loads[:6]:
        one.start()
    for d in range(1, hops + 1):
        @pl.when(me - d < 0)
        def _():
            before[hops - d] = jnp.zeros((rows, D), BF16)

        @pl.when(me + d >= count)
        def _():
            q_all[d] = jnp.zeros((rows, D), BF16)
            cot_after[d - 1] = jnp.zeros((rows, D), BF16)
            stats_after[d - 1] = jnp.zeros(stats.shape, F32)

    extra = pooled.shape[0] - total
    pooled[pl.ds(total, extra), :] = jnp.zeros((extra, D), F32)
    cg_all[pl.ds(count, extra // outs)] = jnp.zeros((extra // outs, outs, D), BF16)
    for ref in (uq2, fq2, uk2, fk2, v2, g2):
        ref[pl.ds(total, extra), :] = jnp.zeros((extra, ref.shape[1]), F32)
    loads[6].wait()
    loads[7].wait()
    groups = (iota((outs, rows), 1) // POOL == iota((outs, rows), 0)).astype(F32).astype(BF16)
    cg_own[...] = dot(groups, cot_ref[...]).astype(BF16)
    own = x_ref[...].astype(F32)
    own_b = rms_rows(own)[0].astype(BF16)
    down = Halo(x_ref, before, halo_sends.at[0], halo_recvs.at[0], hops, 1)
    up_cot = Halo(cot_ref, cot_after, halo_sends.at[1], halo_recvs.at[1], hops, -1)
    up = Halo(q_all.at[0], q_all.at[pl.ds(1, hops)], halo_sends.at[2], halo_recvs.at[2], hops, -1)
    cg_spread = Spread(cg_own, cg_all, *sems[:4])
    pool_spread = Spread(pool_own, pool_all, *sems[4:])
    met_all()
    down.start()
    cg_spread.start()
    up_cot.start()
    loads[0].wait()
    unit, factor = head_rms(dot(own_b, w_ref[1]))
    k_all[pl.ds(margin, rows), :] = unit.astype(BF16)
    unit_k[...] = unit
    scale_k[...] = factor
    loads[1].wait()
    v_all[pl.ds(margin, rows), :] = dot(own_b, w_ref[2]).astype(BF16)
    loads[2].wait()
    unit, factor = head_rms(dot(own_b, w_ref[0]))
    q_all[0] = (unit * QUERY).astype(BF16)
    unit_q[...] = unit
    scale_q[...] = factor

    def keys(d):
        slot = pl.ds(margin - d * rows, rows)
        prev = rms_rows(before[hops - d].astype(F32))[0].astype(BF16)
        k_all[slot, :] = head_rms(dot(prev, w_ref[1]))[0].astype(BF16)
        v_all[slot, :] = dot(prev, w_ref[2]).astype(BF16)

    masks = window_masks(hops, rows, me)

    def scores(p, low, high):
        cols = pl.ds(p * PAIR, PAIR)
        span = pl.ds(low * rows, (high - low) * rows)
        s = dot_nt(both(q_all[0, :, cols]), k_all[span, cols])
        e = [
            jnp.where(masks[b], jnp.exp2(s[:, (b - low) * rows : (b - low + 1) * rows]), 0.0)
            for b in range(low, high)
        ]
        e_b = jnp.concatenate(e, axis=1).astype(BF16)
        e_ref[p, :, span] = e_b
        return functools.reduce(jnp.add, e), dot(e_b, v_all[span, cols])

    half = hops // 2
    for d in range(1, hops - half + 1):
        down.land(d)
        keys(d)
    cg_spread.widen()
    for p in range(HEADS // 2):
        t_ref[p], acc_ref[p] = scores(p, half, hops + 1)
    for d in range(hops - half + 1, hops + 1):
        down.land(d)
        keys(d)
    cg_spread.cross()
    lane = iota((rows, 128), 1)
    totals = jnp.ones((rows, 128), F32)
    for p in range(HEADS // 2):
        t, acc = scores(p, 0, half)
        t = jnp.sum(t + t_ref[p], axis=-1, keepdims=True)
        inverse = jnp.broadcast_to(1.0 / t, (2 * rows, PAIR))
        rt_ref[p] = inverse
        att_ref[:, pl.ds(p * PAIR, PAIR)] = pick((acc + acc_ref[p]) * inverse).astype(BF16)
        totals = jnp.where(lane == 2 * p, t[:rows], totals)
        totals = jnp.where(lane == 2 * p + 1, t[rows:], totals)
    loads[3].wait()
    hidden = (own + dot(att_ref[...], out_w[...])).astype(BF16)
    hidden_ref[...] = hidden
    back = iota((outs, rows), 0) * POOL - iota((outs, rows), 1)
    part = dot(((back >= 0) & (back < POOL)).astype(F32).astype(BF16), hidden)
    tail = dot((iota((outs, rows), 1) > rows - POOL).astype(F32).astype(BF16), hidden)
    lanes = D // outs
    folded = jnp.zeros((outs, lanes), F32)
    for c in range(outs):
        folded = jnp.where(iota((outs, lanes), 0) == c, tail[:, c * lanes : (c + 1) * lanes], folded)
    pool_own[...] = (jnp.concatenate([part, folded], axis=1) / POOL).astype(BF16)
    pool_spread.start()
    cg_spread.finish()
    up_cot.finish()
    loads[4].wait()
    loads[5].wait()
    base = seq * subs * outs
    span = (subs - 1) * outs + far
    coarse = Coarse(total, span, base, cw, cow, (uq2, fq2, uk2, fk2, v2, g2))
    coarse.grads(cg_all[pl.ds(0, count)].astype(F32).reshape(total, D).astype(BF16))
    gcot[pl.ds(0, rows), :] = dot_nt(cot_ref[...], out_w[...])
    gcot[pl.ds(rows, margin), :] = dot_nt(cot_after[...].reshape(margin, D), out_w[...])
    stats[pl.ds(0, HEADS), :] = jnp.log2(totals.T[:HEADS])
    pool_spread.widen()
    pool_spread.cross()
    pool_spread.finish()
    up.start()
    got = pool_all[...].astype(F32).reshape(total, D + lanes)
    block = min(total, 256)
    place_at = (iota((block, block), 0) // outs == iota((block, block), 1) // outs) & (iota((block, block), 0) % outs == 0)
    place_at = place_at.astype(F32).astype(BF16)
    tails = []
    for i in range(total // block):
        one = got[i * block : (i + 1) * block, D:]
        wide = [jnp.where(iota(one.shape, 0) % outs == c, one, 0.0) for c in range(outs)]
        tails.append(dot(place_at, jnp.concatenate(wide, axis=1).astype(BF16)))
    tails = jnp.concatenate([jnp.zeros((outs, D), F32)] + tails)[:total]
    pooled_v = (got[:, :D] + tails).astype(BF16).astype(F32)
    pooled[pl.ds(0, total), :] = pooled_v
    coarse.project(rms_rows(pooled_v)[0].astype(BF16))
    mixed, ng = coarse.finish(subs * outs)
    mixed_ref[...] = mixed
    ng_ref[...] = ng

    def cut(sub):
        start = pl.multiple_of(sub * outs, outs)
        return mixed_ref[pl.ds(start, outs), :], ng_ref[pl.ds(start, far), :]

    copies = []
    for k in range(1, subs):
        other = (mine + k) % subs
        x_out[k] = jnp.concatenate(cut(other)).astype(BF16)
        copies.append(remote(
            x_out.at[k], x_in.at[k], x_sems.at[0, k], x_sems.at[1, k], seq * subs + other, subs
        ))
        copies[-1].start()
    mixed, ng = cut(mine)
    start = pl.multiple_of(me * outs, outs)
    pooled_own = pooled[pl.ds(start, far), :]
    cg = cg_all[pl.ds(me, far // outs)].astype(F32).reshape(far, D)
    normed, factor = rms_rows(pooled_own)
    for copy in copies:
        copy.wait()
    for k in range(1, subs):
        other = x_in[k].astype(F32)
        mixed, ng = mixed + other[:outs], ng + other[outs:]
    pg = (cg + row_back(ng, normed, factor)) / POOL
    pg = jnp.where(me * outs + iota(pg.shape, 0) < total, pg, 0.0).astype(BF16)
    pgw = dot_nt(pg, out_w[...]).astype(BF16)
    lift = ((iota((length, far), 0) + POOL - 1) // POOL == iota((length, far), 1)).astype(F32).astype(BF16)
    g_all[...] = (gcot[...] + dot(lift, pgw)).astype(BF16)
    delta = head_sum(g_all[pl.ds(0, rows), :].astype(F32) * att_ref[...].astype(F32))
    stats[pl.ds(HEADS, HEADS), :] = delta.T[:HEADS]
    moves = [
        Shift(stats, stats_after.at[d - 1], stat_sems.at[0, d - 1], stat_sems.at[1, d - 1], -d)
        for d in range(1, hops + 1)
    ]
    for move in moves:
        move.start()
    state = (pooled_own[:outs] + mixed).astype(BF16)
    onto = (iota((rows, outs), 0) // POOL == iota((rows, outs), 1)).astype(F32).astype(BF16)
    output_ref[...] = (hidden_ref[...].astype(F32) + dot(onto, state)).astype(BF16)
    for p in range(HEADS // 2):
        cols = pl.ds(p * PAIR, PAIR)
        dp = dot_nt(both(g_all[pl.ds(0, rows), cols]), v_all[:, cols])
        column = jnp.concatenate([delta[:, 2 * p : 2 * p + 1], delta[:, 2 * p + 1 : 2 * p + 2]])
        ds = (e_ref[p].astype(F32) * (dp - column)).astype(BF16)
        dq_ref[:, cols] = pick(dot(ds, k_all[:, cols]) * rt_ref[p]) * SCALE
    up.finish()
    for move in moves:
        move.wait()
    gap = iota((rows, length), 1) - iota((rows, length), 0)
    mask_t = (gap >= 0) & (gap < WINDOW)
    every = jnp.concatenate([stats[...]] + [stats_after[d] for d in range(hops)], axis=1)
    dk_p, dv_p = [], []
    for p in range(HEADS // 2):
        cols = pl.ds(p * PAIR, PAIR)
        own_slot = pl.ds(margin, rows)
        qp, gp = q_all[:, :, cols].reshape(length, PAIR), g_all[:, cols]
        st = dot_nt(both(k_all[own_slot, cols]), qp)
        dpt = dot_nt(both(v_all[own_slot, cols]), gp)
        pts, dsts = [], []
        for h in range(2):
            head = 2 * p + h
            part = slice(h * rows, (h + 1) * rows)
            pt = jnp.where(mask_t, jnp.exp2(st[part] - every[head : head + 1]), 0.0)
            pts.append(pt.astype(BF16))
            dsts.append((pt * (dpt[part] - every[HEADS + head : HEADS + head + 1])).astype(BF16))
        dk_p.append(pick(dot(jnp.concatenate(dsts), qp)) * LN2)
        dv_p.append(pick(dot(jnp.concatenate(pts), gp)))
    join = lambda parts: jnp.concatenate(parts, axis=1)
    dq = head_back(dq_ref[...], unit_q[...], scale_q[...]).astype(BF16)
    dk = head_back(join(dk_p), unit_k[...], scale_k[...]).astype(BF16)
    dv = join(dv_p).astype(BF16)
    grads = dot_nt(dq, w_ref[0]) + dot_nt(dk, w_ref[1]) + dot_nt(dv, w_ref[2])
    normed, factor = rms_rows(x_ref[...].astype(F32))
    hidden_grad = cot_ref[...].astype(F32) + dot(lift[:rows], pg)
    grad_ref[...] = (hidden_grad + row_back(grads, normed, factor)).astype(BF16)
    down.drain()
    up_cot.drain()
    up.drain()


def per_device(tokens, cotangent, fine_qkv, fine_out, coarse_qkv, coarse_out):
    rows = tokens.shape[0]
    hops = -(-WINDOW // rows)
    outs = rows // POOL
    me, count, subs = place()
    far = (hops + 2) * outs
    length = (hops + 1) * rows
    total = count * outs
    span = (subs - 1) * outs + far
    width = coarse_qkv.shape[2]
    pairs = HEADS // 2
    shape = jax.ShapeDtypeStruct
    dma = pltpu.SemaphoreType.DMA
    vmem = pltpu.VMEM
    fine_w = jnp.transpose(fine_qkv, (1, 0, 2))
    coarse_w = jnp.transpose(coarse_qkv, (1, 0, 2))
    wide = D + D // outs
    padded = total + far
    scratch = [
        vmem((rows, D), BF16), vmem((rows, D), BF16),
        vmem(fine_w.shape, BF16), vmem(fine_out.shape, BF16), vmem(coarse_w.shape, BF16),
        vmem(coarse_out.shape, BF16),
        vmem((hops, rows, D), BF16), vmem((hops + 1, rows, D), BF16), vmem((hops, rows, D), BF16),
        vmem((length, D), BF16), vmem((length, D), BF16),
        vmem((rows, D), F32), vmem((rows, D), F32), vmem((rows, D), F32), vmem((rows, D), F32),
        vmem((pairs, 2 * rows, length), BF16), vmem((pairs, 2 * rows, rows), F32),
        vmem((pairs, 2 * rows, PAIR), F32), vmem((pairs, 2 * rows, PAIR), F32),
        vmem((rows, D), BF16), vmem((rows, D), BF16),
        vmem((outs, D), BF16), vmem((count + far // outs, outs, D), BF16),
        vmem((outs, wide), BF16), vmem((count, outs, wide), BF16),
        vmem((padded, D), F32), vmem((length, D), F32), vmem((length, D), BF16),
    ] + [vmem((padded, width), F32)] * 6 + [
        vmem((subs * outs, D), F32), vmem((span, D), F32),
        vmem((subs, outs + far, D), BF16), vmem((subs, outs + far, D), BF16),
        vmem((2 * HEADS, rows), F32), vmem((hops, 2 * HEADS, rows), F32), vmem((rows, D), F32),
        dma((8,)), dma((3, 2 * hops)), dma((3, hops)), dma((2, subs)), dma((2, hops)),
    ] + spread_sems(count, subs) * 2
    return pl.pallas_call(
        functools.partial(layer_pair, hops),
        out_shape=[shape((rows, D), BF16)] * 2,
        in_specs=[HBM] * 6,
        out_specs=[VMEM] * 2,
        scratch_shapes=scratch,
        compiler_params=pltpu.CompilerParams(
            collective_id=0, has_side_effects=True, vmem_limit_bytes=(48 if total <= 1024 else 63) * 1024 * 1024
        ),
    )(*[
        pltpu.with_memory_space_constraint(a, pltpu.HBM)
        for a in (tokens, cotangent, fine_w, fine_out, coarse_w, coarse_out)
    ])


def solution(mesh):
    placed = (
        P(("seq", "sub"), None),
        P(("seq", "sub"), None),
        P(),
        P(),
        P(None, None, "sub"),
        P("sub", None),
    )
    return jax.shard_map(
        per_device,
        mesh=mesh,
        in_specs=placed,
        out_specs=(P(("seq", "sub"), None), P(("seq", "sub"), None)),
        check_vma=False,
    )
```

```python
import functools
import math

import jax
import jax.numpy as jnp
from jax import lax
from jax.experimental import pallas as pl
from jax.experimental.pallas import tpu as pltpu
from jax.sharding import PartitionSpec as P

D = 1024
HEADS = 16
HEAD_DIM = 64
WINDOW = 512
POOL = 16
PIECES = 4
EPS = 1e-06
F32 = jnp.float32
BF16 = jnp.bfloat16
MESH = pl.DeviceIdType.MESH
PAIR = 2 * HEAD_DIM
SCALE = HEAD_DIM ** (-0.5)
LN2 = math.log(2.0)
QUERY = SCALE / LN2
VMEM = pl.BlockSpec(memory_space=pltpu.VMEM)
HBM = pl.BlockSpec(memory_space=pltpu.HBM)
SMEM = pl.BlockSpec(memory_space=pltpu.SMEM)


def dot(a, b):
    return jnp.dot(a, b, preferred_element_type=F32)


def dot_nt(a, b):
    return lax.dot_general(a, b, (((1,), (1,)), ((), ())), preferred_element_type=F32)


def dot_tn(a, b):
    return lax.dot_general(a, b, (((0,), (0,)), ((), ())), preferred_element_type=F32)


def split(x):
    hi = x.astype(BF16)
    return hi, (x - hi.astype(F32)).astype(BF16)


def iota(shape, axis):
    return lax.broadcasted_iota(jnp.int32, shape, axis)


def head_sum(x):
    group = (iota((x.shape[1], 128), 0) // HEAD_DIM == iota((x.shape[1], 128), 1)).astype(F32).astype(BF16)
    hi, lo = split(x)
    return dot(hi, group) + dot(lo, group)


def head_mean(x):
    group = iota((PAIR, PAIR), 0) // HEAD_DIM == iota((PAIR, PAIR), 1) // HEAD_DIM
    group = jnp.where(group, 1.0 / HEAD_DIM, 0.0).astype(BF16)
    x = x.astype(BF16)
    return jnp.concatenate([dot(x[:, c : c + PAIR], group) for c in range(0, x.shape[1], PAIR)], axis=1)


def head_rms(raw):
    factor = lax.rsqrt(head_mean(raw * raw) + EPS)
    return raw * factor, factor


def head_back(grad, unit, factor):
    return factor * (grad - unit * head_mean(unit * grad))


def rms_rows(x):
    factor = lax.rsqrt(jnp.mean(x * x, axis=-1, keepdims=True) + EPS)
    return x * factor, factor


def row_back(grad, normed, factor):
    return factor * (grad - normed * jnp.mean(normed * grad, axis=-1, keepdims=True))


def both(pair):
    low = iota(pair.shape, 1) < HEAD_DIM
    wide = pair.astype(F32)
    return jnp.concatenate([jnp.where(low, wide, 0.0), jnp.where(low, 0.0, wide)]).astype(BF16)


def pick(stacked):
    half = stacked.shape[0] // 2
    low = iota((half, PAIR), 1) < HEAD_DIM
    return jnp.where(low, stacked[:half], stacked[half:])


def place():
    subs = lax.axis_size("sub")
    count = lax.axis_size("seq") * subs
    me = lax.axis_index("seq") * subs + lax.axis_index("sub")
    return me, count, subs


def coords(index, subs):
    return (index // subs, index % subs)


def greet_all():
    me, count, subs = place()
    barrier = pltpu.get_barrier_semaphore()

    @pl.loop(1, count)
    def _(k):
        pl.semaphore_signal(
            barrier, inc=1, device_id=coords((me + k) % count, subs), device_id_type=MESH
        )


def met_all():
    pl.semaphore_wait(pltpu.get_barrier_semaphore(), lax.axis_size("seq") * lax.axis_size("sub") - 1)


def remote(src, dst, send, recv, target, subs):
    return pltpu.make_async_remote_copy(
        src_ref=src, dst_ref=dst, send_sem=send, recv_sem=recv,
        device_id=coords(target, subs), device_id_type=MESH,
    )


class Spread:
    def __init__(self, src, dst, out_sem, mid_sem, last_sem, sent):
        self.me, self.count, self.subs = place()
        self.cores = 2 if lax.axis_size("seq") % 2 == 0 else 1
        self.groups = self.count // self.subs // self.cores
        self.sub = self.me % self.subs
        self.core = self.me // self.subs % self.cores
        self.group = self.me // self.subs // self.cores
        self.src, self.dst, self.sems, self.sent = src, dst, (out_sem, mid_sem, last_sem), sent

    def index(self, k, core, j):
        group = (self.group + self.groups - k) % self.groups
        sub = (self.sub + self.subs - j) % self.subs
        return (group * self.cores + (self.core + core) % self.cores) * self.subs + sub

    def copy(self, phase, j, k):
        if phase == 0:
            spot, source = self.me, self.src
            target, sem = self.index(self.groups - k, 0, 0), self.sems[0].at[k]
        elif phase == 1:
            spot = self.index(k, 0, 0)
            target, sem = self.index(0, 0, self.subs - j), self.sems[1].at[j, k]
        else:
            spot = self.index(k, 0, j)
            target, sem = self.index(0, 1, 0), self.sems[2].at[j, k]
        source = self.src if phase == 0 else self.dst.at[spot]
        return remote(source, self.dst.at[spot], self.sent.at[phase, j, k], sem, target, self.subs)

    def arrive(self, phase, j, k):
        if phase == 0:
            spot, sem = self.index(k, 0, 0), self.sems[0].at[k]
        elif phase == 1:
            spot, sem = self.index(k, 0, j), self.sems[1].at[j, k]
        else:
            spot, sem = self.index(k, 1, j), self.sems[2].at[j, k]
        other = (self.me + 1) % self.count
        return remote(self.dst.at[spot], self.dst.at[spot], self.sent.at[phase, j, k], sem, other, self.subs)

    def relay(self, k):
        for j in range(1, self.subs):
            self.copy(1, j, k).start()
        if self.cores > 1:
            self.copy(2, 0, k).start()

    def start(self):
        self.dst[self.me] = self.src[...]

        @pl.loop(1, self.groups)
        def _(k):
            self.copy(0, 0, k).start()

        self.relay(0)

    def widen(self):
        @pl.loop(1, self.groups)
        def _(k):
            self.arrive(0, 0, k).wait_recv()
            self.relay(k)

    def cross(self):
        @pl.loop(0, self.groups)
        def _(k):
            for j in range(1, self.subs):
                self.arrive(1, j, k).wait_recv()
                if self.cores > 1:
                    self.copy(2, j, k).start()

    def finish(self):
        @pl.loop(0, self.groups)
        def _(k):
            for j in range(self.subs):
                if self.cores > 1:
                    self.arrive(2, j, k).wait_recv()
                    self.copy(2, j, k).wait_send()
                if j > 0:
                    self.copy(1, j, k).wait_send()

        @pl.loop(1, self.groups)
        def _(k):
            self.copy(0, 0, k).wait_send()


def spread_sems(count, subs):
    cores = 2 if count // subs % 2 == 0 else 1
    groups = count // subs // cores
    dma = pltpu.SemaphoreType.DMA
    return [dma((groups,)), dma((subs, groups)), dma((subs, groups)), dma((3, subs, groups))]


class Halo:
    def __init__(self, src, dst, sends, recvs, hops, sign):
        self.me, self.count, self.subs = place()
        self.src, self.dst, self.sends, self.recvs = src, dst, sends, recvs
        self.hops, self.sign = hops, sign
        self.paired = lax.axis_size("seq") % 2 == 0
        far_core = self.me // self.subs % 2
        self.first = far_core == (0 if sign > 0 else 1)

    def slot(self, d):
        return self.dst.at[self.hops - d if self.sign > 0 else d - 1]

    def inside(self, index):
        return (index >= 0) & (index < self.count)

    def cuts(self, d):
        if not self.paired or d <= self.subs:
            return self.inside(self.me + self.sign * d)
        target = self.me + self.sign * d + 2 * self.count * self.subs
        core = target // self.subs % 2
        return self.inside(self.me + self.sign * d) & (core == (0 if self.sign > 0 else 1))

    def direct(self, d):
        target = jnp.clip(self.me + self.sign * d, 0, self.count - 1)
        return remote(self.src, self.slot(d), self.sends.at[d - 1], self.recvs.at[d - 1], target, self.subs)

    def passed(self, d):
        target = jnp.clip(self.me + self.sign * self.subs, 0, self.count - 1)
        to = d + self.subs
        return remote(
            self.slot(d), self.slot(to), self.sends.at[self.hops + to - 1], self.recvs.at[to - 1],
            target, self.subs,
        )

    def relays(self, d):
        return self.first & self.inside(self.me - self.sign * d)

    def start(self):
        for d in range(1, self.hops + 1):
            @pl.when(self.cuts(d))
            def _():
                self.direct(d).start()

    def land(self, *near):
        for d in near:
            self.land_one(d)

    def land_one(self, d):
        @pl.when(self.inside(self.me - self.sign * d))
        def _():
            self.direct(d).wait_recv()

        if self.paired and d + self.subs <= self.hops:
            @pl.when(self.relays(d))
            def _():
                self.passed(d).start()

    def stage(self, number):
        if number == 0:
            self.land(*range(1, self.hops + 1))

    def drain(self):
        for d in range(1, self.hops + 1):
            @pl.when(self.cuts(d))
            def _():
                self.direct(d).wait_send()

            if self.paired and d + self.subs <= self.hops:
                @pl.when(self.relays(d))
                def _():
                    self.passed(d).wait_send()


class Braid:
    def __init__(self, src, dst, sends, recvs, hops, sign):
        self.me, self.count, self.subs = place()
        self.src, self.dst, self.sends, self.recvs = src, dst, sends, recvs
        self.hops, self.sign = hops, sign
        self.rank = self.me if sign > 0 else self.count - 1 - self.me
        self.side, self.core = self.rank % 2, self.rank // 2 % 2
        self.size = src.shape[0] // PIECES

    def slot(self, d):
        return self.dst.at[self.hops - d if self.sign > 0 else d - 1]

    def copy(self, kind, source, d, to, slot, piece):
        span = pl.ds(piece * self.size, self.size)
        target = jnp.clip(self.me + self.sign * to, 0, self.count - 1)
        return remote(
            source.at[span], self.slot(slot).at[span], self.sends.at[kind, d - 1, piece],
            self.recvs.at[slot - 1, piece], target, self.subs,
        )

    def direct(self, d, piece):
        return self.copy(0, self.src, d, d, d, piece)

    def across(self, d, piece):
        step = 1 - 2 * self.side
        return self.copy(1, self.slot(d), d, step, d + step, piece)

    def passed(self, d, piece):
        return self.copy(2, self.slot(d), d, 2, d + 2, piece)

    def routes(self):
        near = self.core == 0
        return [
            (self.direct, 2, self.rank + 2 < self.count),
            (self.direct, 4, near & (self.rank + 4 < self.count)),
            (self.direct, 1, (self.rank % 4 != 3) & (self.rank + 1 < self.count)),
            (self.across, 2, near & (self.rank >= 2)),
            (self.across, 4, near & (self.side == 1) & (self.rank >= 4)),
            (self.passed, 1, near & (self.rank >= 1)),
            (self.passed, 2, near & (self.rank >= 2)),
        ]

    def start(self):
        for make, d, used in self.routes()[:3]:
            @pl.when(used)
            def _():
                for piece in range(PIECES):
                    make(d, piece).start()

    def land(self, *near):
        for piece in range(PIECES):
            for d in near:
                @pl.when(self.rank >= d)
                def _():
                    self.direct(d, piece).wait_recv()

                for make, other, used in self.routes()[3:]:
                    if other == d:
                        @pl.when(used)
                        def _():
                            make(d, piece).start()

    def stage(self, number):
        self.land(*((2, 4), (1,), (3,))[number])

    def drain(self):
        for make, d, used in self.routes():
            @pl.when(used)
            def _():
                for piece in range(PIECES):
                    make(d, piece).wait_send()


def braided(hops):
    return lax.axis_size("sub") == 2 and lax.axis_size("seq") % 2 == 0 and hops == 4


def halo(hops, *args):
    return (Braid if braided(hops) else Halo)(*args)


def halo_sems(hops, number):
    dma = pltpu.SemaphoreType.DMA
    if braided(hops):
        return [dma((number, 3, hops, PIECES)), dma((number, hops, PIECES))]
    return [dma((number, 2 * hops)), dma((number, hops))]


class Shift:
    def __init__(self, src, dst, send, recv, distance):
        me, count, subs = place()
        self.me, self.subs, self.target = me, subs, me + distance
        self.args = (src, dst, send, recv)
        self.sends = (me + distance >= 0) & (me + distance < count)
        self.gets = (me - distance >= 0) & (me - distance < count)
        self.copy = remote(src, dst, send, recv, jnp.clip(me + distance, 0, count - 1), subs)

    def start(self):
        @pl.when(self.sends)
        def _():
            self.copy.start()

    def wait(self):
        @pl.when(self.sends)
        def _():
            self.copy.wait_send()

        @pl.when(self.gets)
        def _():
            self.copy.wait_recv()


def window_masks(hops, rows, me):
    margin = hops * rows
    row = iota((2 * rows, rows), 0) % rows
    masks = []
    for b in range(hops + 1):
        least, most = margin - (b + 1) * rows + 1, margin + rows - 1 - b * rows
        gap = margin - b * rows + row - iota((2 * rows, rows), 1)
        mask = jnp.broadcast_to(me - (hops - b), gap.shape) >= 0
        if least < 0:
            mask = mask & (gap >= 0)
        if most >= WINDOW:
            mask = mask & (gap < WINDOW)
        masks.append(mask)
    return masks


def causal(keys, queries):
    return keys <= queries


class Coarse:
    def __init__(self, total, span, base, cw, cow, scratch):
        self.total, self.span, self.base = total, span, base
        self.cw, self.cow = cw, cow
        self.uq, self.fq, self.uk, self.fk, self.v, self.g = scratch
        self.width = cw.shape[2]

    def grads(self, cg):
        self.gb = dot_nt(cg, self.cow[...]).astype(BF16)
        self.g[pl.ds(0, self.total), :] = self.gb.astype(F32)

    def project(self, normed):
        uq, fq = head_rms(dot(normed, self.cw[0]))
        uk, fk = head_rms(dot(normed, self.cw[1]))
        v = dot(normed, self.cw[2])
        for ref, value in ((self.uq, uq), (self.fq, fq), (self.uk, uk), (self.fk, fk), (self.v, v)):
            ref[pl.ds(0, self.total), :] = value
        self.qb, self.kb, self.vb = (uq * QUERY).astype(BF16), uk.astype(BF16), v.astype(BF16)

    def sums(self, cols):
        block = min(self.total, 256)
        inverse, deltas = [], []
        for i in range(self.total // block):
            part = slice(i * block, (i + 1) * block)
            q, g = self.qb[part, cols], self.gb[part, cols]
            t, d = [0.0, 0.0], [0.0, 0.0]
            for j in range(i + 1):
                rows = slice(j * block, (j + 1) * block)
                e = jnp.exp2(dot_nt(both(self.kb[rows, cols]), q))
                if j == i:
                    e = jnp.where(causal(iota(e.shape, 0) % block, iota(e.shape, 1)), e, 0.0)
                ed = e * dot_nt(both(self.vb[rows, cols]), g)
                for h in range(2):
                    half = slice(h * block, (h + 1) * block)
                    t[h] = t[h] + jnp.sum(e[half], axis=0, keepdims=True)
                    d[h] = d[h] + jnp.sum(ed[half], axis=0, keepdims=True)
            inverse.append([1.0 / x for x in t])
            deltas.append([x * r for x, r in zip(d, inverse[-1])])
        join = lambda parts, h: jnp.concatenate([x[h] for x in parts], axis=1)
        return [join(inverse, h) for h in range(2)], [join(deltas, h) for h in range(2)]

    def mine(self, ref, cols):
        start = pl.multiple_of(self.base, 8)
        return ref[pl.ds(start, self.span), cols]

    def attend(self):
        span, total = self.span, self.total
        shape = (2 * span, total)
        own = self.base + iota(shape, 0) % span
        after = causal(own, iota(shape, 1))
        before = causal(iota(shape, 1), own)
        att_p, dq_p, dk_p, dv_p = [], [], [], []
        for p in range(self.width // PAIR):
            cols = slice(p * PAIR, (p + 1) * PAIR)
            inverse, deltas = self.sums(cols)
            ds_cols = pl.ds(p * PAIR, PAIR)
            qp, kp, vp, gp = self.qb[:, cols], self.kb[:, cols], self.vb[:, cols], self.gb[:, cols]
            k2, v2 = both(self.mine(self.uk, ds_cols)), both(self.mine(self.v, ds_cols))
            q2, g2 = both(self.mine(self.uq, ds_cols) * QUERY), both(self.mine(self.g, ds_cols))
            wide = lambda pair: jnp.concatenate([jnp.broadcast_to(x, (span, total)) for x in pair])
            pt = jnp.where(after, jnp.exp2(dot_nt(k2, qp)) * wide(inverse), 0.0)
            dst = pt * (dot_nt(v2, gp) - wide(deltas))
            dk_p.append(pick(dot(dst.astype(BF16), qp)) * LN2)
            dv_p.append(pick(dot(pt.astype(BF16), gp)))
            e = jnp.where(before, jnp.exp2(dot_nt(q2, kp)), 0.0)
            e = e * (1.0 / jnp.sum(e, axis=-1, keepdims=True))
            dp = dot_nt(g2, vp)
            delta = jnp.sum(e * dp, axis=-1, keepdims=True)
            ds = e * (dp - delta)
            dq_p.append(pick(dot(ds.astype(BF16), kp)) * SCALE)
            att_p.append(pick(dot(e.astype(BF16), vp)))
        join = lambda parts: jnp.concatenate(parts, axis=1)
        return join(att_p), join(dq_p), join(dk_p), join(dv_p)

    def finish(self, outs_all):
        every = pl.ds(0, self.width)
        att, dq, dk, dv = self.attend()
        mixed = dot(att[:outs_all].astype(BF16), self.cow[...])
        dq = head_back(dq, self.mine(self.uq, every), self.mine(self.fq, every)).astype(BF16)
        dk = head_back(dk, self.mine(self.uk, every), self.mine(self.fk, every)).astype(BF16)
        dv = dv.astype(BF16)
        return mixed, dot_nt(dq, self.cw[0]) + dot_nt(dk, self.cw[1]) + dot_nt(dv, self.cw[2])


def layer_pair(
    hops, x_hbm, cot_hbm, w_hbm, out_hbm, cw_hbm, cow_hbm, output_ref, grad_ref,
    x_ref, cot_ref,
    w_ref, out_w, cw, cow, before, q_all, cot_after, k_all, v_all,
    unit_q, unit_k, scale_q, scale_k, e_ref, t_ref, acc_ref, rt_ref, att_ref, hidden_ref,
    cg_own, cg_all, pool_own, pool_all, pooled, gcot, g_all,
    uq2, fq2, uk2, fk2, v2, g2, mixed_ref, ng_ref, x_out, x_in, stats, stats_after, dq_ref,
    load, halo_sends, halo_recvs, x_sems, stat_sems, *sems,
):
    me, count, subs = place()
    mine, seq = lax.axis_index("sub"), lax.axis_index("seq")
    rows = x_ref.shape[0]
    outs = rows // POOL
    margin, length = hops * rows, (hops + 1) * rows
    total = count * outs
    far = (hops + 2) * outs
    greet_all()
    parts = [
        (w_hbm.at[1], w_ref.at[1]), (w_hbm.at[2], w_ref.at[2]), (w_hbm.at[0], w_ref.at[0]),
        (out_hbm, out_w), (cw_hbm, cw), (cow_hbm, cow), (x_hbm, x_ref), (cot_hbm, cot_ref),
    ]
    loads = [pltpu.make_async_copy(src, dst, load.at[i]) for i, (src, dst) in enumerate(parts)]
    for one in loads[6:] + loads[:6]:
        one.start()
    for d in range(1, hops + 1):
        @pl.when(me - d < 0)
        def _():
            before[hops - d] = jnp.zeros((rows, D), BF16)

        @pl.when(me + d >= count)
        def _():
            q_all[d] = jnp.zeros((rows, D), BF16)
            cot_after[d - 1] = jnp.zeros((rows, D), BF16)
            stats_after[d - 1] = jnp.zeros(stats.shape, F32)

    extra = pooled.shape[0] - total
    pooled[pl.ds(total, extra), :] = jnp.zeros((extra, D), F32)
    cg_all[pl.ds(count, extra // outs)] = jnp.zeros((extra // outs, outs, D), BF16)
    for ref in (uq2, fq2, uk2, fk2, v2, g2):
        ref[pl.ds(total, extra), :] = jnp.zeros((extra, ref.shape[1]), F32)
    loads[6].wait()
    loads[7].wait()
    groups = (iota((outs, rows), 1) // POOL == iota((outs, rows), 0)).astype(F32).astype(BF16)
    cg_own[...] = dot(groups, cot_ref[...]).astype(BF16)
    own = x_ref[...].astype(F32)
    own_b = rms_rows(own)[0].astype(BF16)
    down = halo(hops, x_ref, before, halo_sends.at[0], halo_recvs.at[0], hops, 1)
    up_cot = halo(hops, cot_ref, cot_after, halo_sends.at[1], halo_recvs.at[1], hops, -1)
    up = halo(hops, q_all.at[0], q_all.at[pl.ds(1, hops)], halo_sends.at[2], halo_recvs.at[2], hops, -1)
    cg_spread = Spread(cg_own, cg_all, *sems[:4])
    pool_spread = Spread(pool_own, pool_all, *sems[4:])
    met_all()
    down.start()
    cg_spread.start()
    up_cot.start()
    loads[0].wait()
    unit, factor = head_rms(dot(own_b, w_ref[1]))
    k_all[pl.ds(margin, rows), :] = unit.astype(BF16)
    unit_k[...] = unit
    scale_k[...] = factor
    loads[1].wait()
    v_all[pl.ds(margin, rows), :] = dot(own_b, w_ref[2]).astype(BF16)
    loads[2].wait()
    unit, factor = head_rms(dot(own_b, w_ref[0]))
    q_all[0] = (unit * QUERY).astype(BF16)
    unit_q[...] = unit
    scale_q[...] = factor

    def keys(d):
        slot = pl.ds(margin - d * rows, rows)
        prev = rms_rows(before[hops - d].astype(F32))[0].astype(BF16)
        k_all[slot, :] = head_rms(dot(prev, w_ref[1]))[0].astype(BF16)
        v_all[slot, :] = dot(prev, w_ref[2]).astype(BF16)

    masks = window_masks(hops, rows, me)

    def scores(p, low, high):
        cols = pl.ds(p * PAIR, PAIR)
        span = pl.ds(low * rows, (high - low) * rows)
        s = dot_nt(both(q_all[0, :, cols]), k_all[span, cols])
        e = [
            jnp.where(masks[b], jnp.exp2(s[:, (b - low) * rows : (b - low + 1) * rows]), 0.0)
            for b in range(low, high)
        ]
        e_b = jnp.concatenate(e, axis=1).astype(BF16)
        e_ref[p, :, span] = e_b
        return functools.reduce(jnp.add, e), dot(e_b, v_all[span, cols])

    half = hops // 2
    if braided(hops):
        down.land(2, 4)
        keys(2)
        keys(4)
        down.land(1)
        up_cot.stage(0)
        keys(1)
        cg_spread.widen()
        for p in range(HEADS // 2):
            t_ref[p], acc_ref[p] = scores(p, half, hops + 1)
        down.land(3)
        up_cot.stage(1)
        keys(3)
    else:
        for d in range(1, hops - half + 1):
            down.land(d)
            keys(d)
        cg_spread.widen()
        for p in range(HEADS // 2):
            t_ref[p], acc_ref[p] = scores(p, half, hops + 1)
        for d in range(hops - half + 1, hops + 1):
            down.land(d)
            keys(d)
        up_cot.stage(0)
        up_cot.stage(1)
    cg_spread.cross()
    lane = iota((rows, 128), 1)
    totals = jnp.ones((rows, 128), F32)
    for p in range(HEADS // 2):
        t, acc = scores(p, 0, half)
        t = jnp.sum(t + t_ref[p], axis=-1, keepdims=True)
        inverse = jnp.broadcast_to(1.0 / t, (2 * rows, PAIR))
        rt_ref[p] = inverse
        att_ref[:, pl.ds(p * PAIR, PAIR)] = pick((acc + acc_ref[p]) * inverse).astype(BF16)
        totals = jnp.where(lane == 2 * p, t[:rows], totals)
        totals = jnp.where(lane == 2 * p + 1, t[rows:], totals)
    loads[3].wait()
    hidden = (own + dot(att_ref[...], out_w[...])).astype(BF16)
    hidden_ref[...] = hidden
    back = iota((outs, rows), 0) * POOL - iota((outs, rows), 1)
    part = dot(((back >= 0) & (back < POOL)).astype(F32).astype(BF16), hidden)
    tail = dot((iota((outs, rows), 1) > rows - POOL).astype(F32).astype(BF16), hidden)
    lanes = D // outs
    folded = jnp.zeros((outs, lanes), F32)
    for c in range(outs):
        folded = jnp.where(iota((outs, lanes), 0) == c, tail[:, c * lanes : (c + 1) * lanes], folded)
    pool_own[...] = (jnp.concatenate([part, folded], axis=1) / POOL).astype(BF16)
    pool_spread.start()
    cg_spread.finish()
    up_cot.stage(2)
    loads[4].wait()
    loads[5].wait()
    base = seq * subs * outs
    span = (subs - 1) * outs + far
    coarse = Coarse(total, span, base, cw, cow, (uq2, fq2, uk2, fk2, v2, g2))
    coarse.grads(cg_all[pl.ds(0, count)].astype(F32).reshape(total, D).astype(BF16))
    gcot[pl.ds(0, rows), :] = dot_nt(cot_ref[...], out_w[...])
    gcot[pl.ds(rows, margin), :] = dot_nt(cot_after[...].reshape(margin, D), out_w[...])
    stats[pl.ds(0, HEADS), :] = jnp.log2(totals.T[:HEADS])
    pool_spread.widen()
    pool_spread.cross()
    pool_spread.finish()
    up.start()
    got = pool_all[...].astype(F32).reshape(total, D + lanes)
    block = min(total, 256)
    place_at = (iota((block, block), 0) // outs == iota((block, block), 1) // outs) & (iota((block, block), 0) % outs == 0)
    place_at = place_at.astype(F32).astype(BF16)
    tails = []
    for i in range(total // block):
        one = got[i * block : (i + 1) * block, D:]
        wide = [jnp.where(iota(one.shape, 0) % outs == c, one, 0.0) for c in range(outs)]
        tails.append(dot(place_at, jnp.concatenate(wide, axis=1).astype(BF16)))
    tails = jnp.concatenate([jnp.zeros((outs, D), F32)] + tails)[:total]
    pooled_v = (got[:, :D] + tails).astype(BF16).astype(F32)
    pooled[pl.ds(0, total), :] = pooled_v
    coarse.project(rms_rows(pooled_v)[0].astype(BF16))
    mixed, ng = coarse.finish(subs * outs)
    mixed_ref[...] = mixed
    ng_ref[...] = ng

    def cut(sub):
        start = pl.multiple_of(sub * outs, outs)
        return mixed_ref[pl.ds(start, outs), :], ng_ref[pl.ds(start, far), :]

    copies = []
    for k in range(1, subs):
        other = (mine + k) % subs
        x_out[k] = jnp.concatenate(cut(other)).astype(BF16)
        copies.append(remote(
            x_out.at[k], x_in.at[k], x_sems.at[0, k], x_sems.at[1, k], seq * subs + other, subs
        ))
        copies[-1].start()
    up.stage(0)
    mixed, ng = cut(mine)
    start = pl.multiple_of(me * outs, outs)
    pooled_own = pooled[pl.ds(start, far), :]
    cg = cg_all[pl.ds(me, far // outs)].astype(F32).reshape(far, D)
    normed, factor = rms_rows(pooled_own)
    for copy in copies:
        copy.wait()
    for k in range(1, subs):
        other = x_in[k].astype(F32)
        mixed, ng = mixed + other[:outs], ng + other[outs:]
    pg = (cg + row_back(ng, normed, factor)) / POOL
    pg = jnp.where(me * outs + iota(pg.shape, 0) < total, pg, 0.0).astype(BF16)
    pgw = dot_nt(pg, out_w[...]).astype(BF16)
    lift = ((iota((length, far), 0) + POOL - 1) // POOL == iota((length, far), 1)).astype(F32).astype(BF16)
    g_all[...] = (gcot[...] + dot(lift, pgw)).astype(BF16)
    delta = head_sum(g_all[pl.ds(0, rows), :].astype(F32) * att_ref[...].astype(F32))
    stats[pl.ds(HEADS, HEADS), :] = delta.T[:HEADS]
    moves = [
        Shift(stats, stats_after.at[d - 1], stat_sems.at[0, d - 1], stat_sems.at[1, d - 1], -d)
        for d in range(1, hops + 1)
    ]
    for move in moves:
        move.start()
    up.stage(1)
    state = (pooled_own[:outs] + mixed).astype(BF16)
    onto = (iota((rows, outs), 0) // POOL == iota((rows, outs), 1)).astype(F32).astype(BF16)
    output_ref[...] = (hidden_ref[...].astype(F32) + dot(onto, state)).astype(BF16)
    for p in range(HEADS // 2):
        cols = pl.ds(p * PAIR, PAIR)
        dp = dot_nt(both(g_all[pl.ds(0, rows), cols]), v_all[:, cols])
        column = jnp.concatenate([delta[:, 2 * p : 2 * p + 1], delta[:, 2 * p + 1 : 2 * p + 2]])
        ds = (e_ref[p].astype(F32) * (dp - column)).astype(BF16)
        dq_ref[:, cols] = pick(dot(ds, k_all[:, cols]) * rt_ref[p]) * SCALE
    up.stage(2)
    for move in moves:
        move.wait()
    gap = iota((rows, length), 1) - iota((rows, length), 0)
    mask_t = (gap >= 0) & (gap < WINDOW)
    every = jnp.concatenate([stats[...]] + [stats_after[d] for d in range(hops)], axis=1)
    dk_p, dv_p = [], []
    for p in range(HEADS // 2):
        cols = pl.ds(p * PAIR, PAIR)
        own_slot = pl.ds(margin, rows)
        qp, gp = q_all[:, :, cols].reshape(length, PAIR), g_all[:, cols]
        st = dot_nt(both(k_all[own_slot, cols]), qp)
        dpt = dot_nt(both(v_all[own_slot, cols]), gp)
        pts, dsts = [], []
        for h in range(2):
            head = 2 * p + h
            part = slice(h * rows, (h + 1) * rows)
            pt = jnp.where(mask_t, jnp.exp2(st[part] - every[head : head + 1]), 0.0)
            pts.append(pt.astype(BF16))
            dsts.append((pt * (dpt[part] - every[HEADS + head : HEADS + head + 1])).astype(BF16))
        dk_p.append(pick(dot(jnp.concatenate(dsts), qp)) * LN2)
        dv_p.append(pick(dot(jnp.concatenate(pts), gp)))
    join = lambda parts: jnp.concatenate(parts, axis=1)
    dq = head_back(dq_ref[...], unit_q[...], scale_q[...]).astype(BF16)
    dk = head_back(join(dk_p), unit_k[...], scale_k[...]).astype(BF16)
    dv = join(dv_p).astype(BF16)
    grads = dot_nt(dq, w_ref[0]) + dot_nt(dk, w_ref[1]) + dot_nt(dv, w_ref[2])
    normed, factor = rms_rows(x_ref[...].astype(F32))
    hidden_grad = cot_ref[...].astype(F32) + dot(lift[:rows], pg)
    grad_ref[...] = (hidden_grad + row_back(grads, normed, factor)).astype(BF16)
    down.drain()
    up_cot.drain()
    up.drain()


def per_device(tokens, cotangent, fine_qkv, fine_out, coarse_qkv, coarse_out):
    rows = tokens.shape[0]
    hops = -(-WINDOW // rows)
    outs = rows // POOL
    me, count, subs = place()
    far = (hops + 2) * outs
    length = (hops + 1) * rows
    total = count * outs
    span = (subs - 1) * outs + far
    width = coarse_qkv.shape[2]
    pairs = HEADS // 2
    shape = jax.ShapeDtypeStruct
    dma = pltpu.SemaphoreType.DMA
    vmem = pltpu.VMEM
    fine_w = jnp.transpose(fine_qkv, (1, 0, 2))
    coarse_w = jnp.transpose(coarse_qkv, (1, 0, 2))
    wide = D + D // outs
    padded = total + far
    scratch = [
        vmem((rows, D), BF16), vmem((rows, D), BF16),
        vmem(fine_w.shape, BF16), vmem(fine_out.shape, BF16), vmem(coarse_w.shape, BF16),
        vmem(coarse_out.shape, BF16),
        vmem((hops, rows, D), BF16), vmem((hops + 1, rows, D), BF16), vmem((hops, rows, D), BF16),
        vmem((length, D), BF16), vmem((length, D), BF16),
        vmem((rows, D), F32), vmem((rows, D), F32), vmem((rows, D), F32), vmem((rows, D), F32),
        vmem((pairs, 2 * rows, length), BF16), vmem((pairs, 2 * rows, rows), F32),
        vmem((pairs, 2 * rows, PAIR), F32), vmem((pairs, 2 * rows, PAIR), F32),
        vmem((rows, D), BF16), vmem((rows, D), BF16),
        vmem((outs, D), BF16), vmem((count + far // outs, outs, D), BF16),
        vmem((outs, wide), BF16), vmem((count, outs, wide), BF16),
        vmem((padded, D), F32), vmem((length, D), F32), vmem((length, D), BF16),
    ] + [vmem((padded, width), F32)] * 6 + [
        vmem((subs * outs, D), F32), vmem((span, D), F32),
        vmem((subs, outs + far, D), BF16), vmem((subs, outs + far, D), BF16),
        vmem((2 * HEADS, rows), F32), vmem((hops, 2 * HEADS, rows), F32), vmem((rows, D), F32),
        dma((8,)), *halo_sems(hops, 3), dma((2, subs)), dma((2, hops)),
    ] + spread_sems(count, subs) * 2
    return pl.pallas_call(
        functools.partial(layer_pair, hops),
        out_shape=[shape((rows, D), BF16)] * 2,
        in_specs=[HBM] * 6,
        out_specs=[VMEM] * 2,
        scratch_shapes=scratch,
        compiler_params=pltpu.CompilerParams(
            collective_id=0, has_side_effects=True, vmem_limit_bytes=(48 if total <= 1024 else 63) * 1024 * 1024
        ),
    )(*[
        pltpu.with_memory_space_constraint(a, pltpu.HBM)
        for a in (tokens, cotangent, fine_w, fine_out, coarse_w, coarse_out)
    ])


def solution(mesh):
    placed = (
        P(("seq", "sub"), None),
        P(("seq", "sub"), None),
        P(),
        P(),
        P(None, None, "sub"),
        P("sub", None),
    )
    return jax.shard_map(
        per_device,
        mesh=mesh,
        in_specs=placed,
        out_specs=(P(("seq", "sub"), None), P(("seq", "sub"), None)),
        check_vma=False,
    )
```

```python
import functools
import math

import jax
import jax.numpy as jnp
from jax import lax
from jax.experimental import pallas as pl
from jax.experimental.pallas import tpu as pltpu
from jax.sharding import PartitionSpec as P

D = 1024
HEADS = 16
HEAD_DIM = 64
WINDOW = 512
POOL = 16
PIECES = 4
EPS = 1e-06
F32 = jnp.float32
BF16 = jnp.bfloat16
MESH = pl.DeviceIdType.MESH
PAIR = 2 * HEAD_DIM
SCALE = HEAD_DIM ** (-0.5)
LN2 = math.log(2.0)
QUERY = SCALE / LN2
VMEM = pl.BlockSpec(memory_space=pltpu.VMEM)
HBM = pl.BlockSpec(memory_space=pltpu.HBM)
SMEM = pl.BlockSpec(memory_space=pltpu.SMEM)


def dot(a, b):
    return jnp.dot(a, b, preferred_element_type=F32)


def dot_nt(a, b):
    return lax.dot_general(a, b, (((1,), (1,)), ((), ())), preferred_element_type=F32)


def dot_tn(a, b):
    return lax.dot_general(a, b, (((0,), (0,)), ((), ())), preferred_element_type=F32)


def split(x):
    hi = x.astype(BF16)
    return hi, (x - hi.astype(F32)).astype(BF16)


def iota(shape, axis):
    return lax.broadcasted_iota(jnp.int32, shape, axis)


def head_sum(x):
    group = (iota((x.shape[1], 128), 0) // HEAD_DIM == iota((x.shape[1], 128), 1)).astype(F32).astype(BF16)
    hi, lo = split(x)
    return dot(hi, group) + dot(lo, group)


def head_mean(x):
    group = iota((PAIR, PAIR), 0) // HEAD_DIM == iota((PAIR, PAIR), 1) // HEAD_DIM
    group = jnp.where(group, 1.0 / HEAD_DIM, 0.0).astype(BF16)
    x = x.astype(BF16)
    return jnp.concatenate([dot(x[:, c : c + PAIR], group) for c in range(0, x.shape[1], PAIR)], axis=1)


def head_rms(raw):
    factor = lax.rsqrt(head_mean(raw * raw) + EPS)
    return raw * factor, factor


def head_back(grad, unit, factor):
    return factor * (grad - unit * head_mean(unit * grad))


def rms_rows(x):
    factor = lax.rsqrt(jnp.mean(x * x, axis=-1, keepdims=True) + EPS)
    return x * factor, factor


def row_back(grad, normed, factor):
    return factor * (grad - normed * jnp.mean(normed * grad, axis=-1, keepdims=True))


def both(pair):
    low = iota(pair.shape, 1) < HEAD_DIM
    wide = pair.astype(F32)
    return jnp.concatenate([jnp.where(low, wide, 0.0), jnp.where(low, 0.0, wide)]).astype(BF16)


def pick(stacked):
    half = stacked.shape[0] // 2
    low = iota((half, PAIR), 1) < HEAD_DIM
    return jnp.where(low, stacked[:half], stacked[half:])


def place():
    subs = lax.axis_size("sub")
    count = lax.axis_size("seq") * subs
    me = lax.axis_index("seq") * subs + lax.axis_index("sub")
    return me, count, subs


def coords(index, subs):
    return (index // subs, index % subs)


def greet_all():
    me, count, subs = place()
    barrier = pltpu.get_barrier_semaphore()

    @pl.loop(1, count)
    def _(k):
        pl.semaphore_signal(
            barrier, inc=1, device_id=coords((me + k) % count, subs), device_id_type=MESH
        )


def met_all():
    pl.semaphore_wait(pltpu.get_barrier_semaphore(), lax.axis_size("seq") * lax.axis_size("sub") - 1)


def remote(src, dst, send, recv, target, subs):
    return pltpu.make_async_remote_copy(
        src_ref=src, dst_ref=dst, send_sem=send, recv_sem=recv,
        device_id=coords(target, subs), device_id_type=MESH,
    )


class Spread:
    def __init__(self, src, dst, out_sem, mid_sem, last_sem, sent):
        self.me, self.count, self.subs = place()
        self.cores = 2 if lax.axis_size("seq") % 2 == 0 else 1
        self.groups = self.count // self.subs // self.cores
        self.sub = self.me % self.subs
        self.core = self.me // self.subs % self.cores
        self.group = self.me // self.subs // self.cores
        self.src, self.dst, self.sems, self.sent = src, dst, (out_sem, mid_sem, last_sem), sent

    def index(self, k, core, j):
        group = (self.group + self.groups - k) % self.groups
        sub = (self.sub + self.subs - j) % self.subs
        return (group * self.cores + (self.core + core) % self.cores) * self.subs + sub

    def copy(self, phase, j, k):
        if phase == 0:
            spot, source = self.me, self.src
            target, sem = self.index(self.groups - k, 0, 0), self.sems[0].at[k]
        elif phase == 1:
            spot = self.index(k, 0, 0)
            target, sem = self.index(0, 0, self.subs - j), self.sems[1].at[j, k]
        else:
            spot = self.index(k, 0, j)
            target, sem = self.index(0, 1, 0), self.sems[2].at[j, k]
        source = self.src if phase == 0 else self.dst.at[spot]
        return remote(source, self.dst.at[spot], self.sent.at[phase, j, k], sem, target, self.subs)

    def arrive(self, phase, j, k):
        if phase == 0:
            spot, sem = self.index(k, 0, 0), self.sems[0].at[k]
        elif phase == 1:
            spot, sem = self.index(k, 0, j), self.sems[1].at[j, k]
        else:
            spot, sem = self.index(k, 1, j), self.sems[2].at[j, k]
        other = (self.me + 1) % self.count
        return remote(self.dst.at[spot], self.dst.at[spot], self.sent.at[phase, j, k], sem, other, self.subs)

    def relay(self, k):
        for j in range(1, self.subs):
            self.copy(1, j, k).start()
        if self.cores > 1:
            self.copy(2, 0, k).start()

    def start(self):
        self.dst[self.me] = self.src[...]

        @pl.loop(1, self.groups)
        def _(k):
            self.copy(0, 0, k).start()

        self.relay(0)

    def widen(self):
        @pl.loop(1, self.groups)
        def _(k):
            self.arrive(0, 0, k).wait_recv()
            self.relay(k)

    def cross(self):
        @pl.loop(0, self.groups)
        def _(k):
            for j in range(1, self.subs):
                self.arrive(1, j, k).wait_recv()
                if self.cores > 1:
                    self.copy(2, j, k).start()

    def finish(self):
        @pl.loop(0, self.groups)
        def _(k):
            for j in range(self.subs):
                if self.cores > 1:
                    self.arrive(2, j, k).wait_recv()
                    self.copy(2, j, k).wait_send()
                if j > 0:
                    self.copy(1, j, k).wait_send()

        @pl.loop(1, self.groups)
        def _(k):
            self.copy(0, 0, k).wait_send()


def spread_sems(count, subs):
    cores = 2 if count // subs % 2 == 0 else 1
    groups = count // subs // cores
    dma = pltpu.SemaphoreType.DMA
    return [dma((groups,)), dma((subs, groups)), dma((subs, groups)), dma((3, subs, groups))]


class Halo:
    def __init__(self, src, dst, sends, recvs, hops, sign):
        self.me, self.count, self.subs = place()
        self.src, self.dst, self.sends, self.recvs = src, dst, sends, recvs
        self.hops, self.sign = hops, sign
        self.paired = lax.axis_size("seq") % 2 == 0
        far_core = self.me // self.subs % 2
        self.first = far_core == (0 if sign > 0 else 1)

    def slot(self, d):
        return self.dst.at[self.hops - d if self.sign > 0 else d - 1]

    def inside(self, index):
        return (index >= 0) & (index < self.count)

    def cuts(self, d):
        if not self.paired or d <= self.subs:
            return self.inside(self.me + self.sign * d)
        target = self.me + self.sign * d + 2 * self.count * self.subs
        core = target // self.subs % 2
        return self.inside(self.me + self.sign * d) & (core == (0 if self.sign > 0 else 1))

    def direct(self, d):
        target = jnp.clip(self.me + self.sign * d, 0, self.count - 1)
        return remote(self.src, self.slot(d), self.sends.at[d - 1], self.recvs.at[d - 1], target, self.subs)

    def passed(self, d):
        target = jnp.clip(self.me + self.sign * self.subs, 0, self.count - 1)
        to = d + self.subs
        return remote(
            self.slot(d), self.slot(to), self.sends.at[self.hops + to - 1], self.recvs.at[to - 1],
            target, self.subs,
        )

    def relays(self, d):
        return self.first & self.inside(self.me - self.sign * d)

    def start(self):
        for d in range(1, self.hops + 1):
            @pl.when(self.cuts(d))
            def _():
                self.direct(d).start()

    def land(self, *near):
        for d in near:
            self.land_one(d)

    def land_one(self, d):
        @pl.when(self.inside(self.me - self.sign * d))
        def _():
            self.direct(d).wait_recv()

        if self.paired and d + self.subs <= self.hops:
            @pl.when(self.relays(d))
            def _():
                self.passed(d).start()

    def stage(self, number):
        if number == 0:
            self.land(*range(1, self.hops + 1))

    def drain(self):
        for d in range(1, self.hops + 1):
            @pl.when(self.cuts(d))
            def _():
                self.direct(d).wait_send()

            if self.paired and d + self.subs <= self.hops:
                @pl.when(self.relays(d))
                def _():
                    self.passed(d).wait_send()


class Braid:
    def __init__(self, src, dst, sends, recvs, hops, sign):
        self.me, self.count, self.subs = place()
        self.src, self.dst, self.sends, self.recvs = src, dst, sends, recvs
        self.hops, self.sign = hops, sign
        self.rank = self.me if sign > 0 else self.count - 1 - self.me
        self.side, self.core = self.rank % 2, self.rank // 2 % 2
        self.size = src.shape[0] // PIECES

    def slot(self, d):
        return self.dst.at[self.hops - d if self.sign > 0 else d - 1]

    def copy(self, kind, source, d, to, slot, piece):
        span = pl.ds(piece * self.size, self.size)
        target = jnp.clip(self.me + self.sign * to, 0, self.count - 1)
        return remote(
            source.at[span], self.slot(slot).at[span], self.sends.at[kind, d - 1, piece],
            self.recvs.at[slot - 1, piece], target, self.subs,
        )

    def direct(self, d, piece):
        return self.copy(0, self.src, d, d, d, piece)

    def across(self, d, piece):
        step = 1 - 2 * self.side
        return self.copy(1, self.slot(d), d, step, d + step, piece)

    def passed(self, d, piece):
        return self.copy(2, self.slot(d), d, 2, d + 2, piece)

    def routes(self):
        near = self.core == 0
        return [
            (self.direct, 2, self.rank + 2 < self.count),
            (self.direct, 4, near & (self.rank + 4 < self.count)),
            (self.direct, 1, (self.rank % 4 != 3) & (self.rank + 1 < self.count)),
            (self.across, 2, near & (self.rank >= 2)),
            (self.across, 4, near & (self.side == 1) & (self.rank >= 4)),
            (self.passed, 1, near & (self.rank >= 1)),
            (self.passed, 2, near & (self.rank >= 2)),
        ]

    def start(self):
        for make, d, used in self.routes()[:3]:
            @pl.when(used)
            def _():
                for piece in range(PIECES):
                    make(d, piece).start()

    def land(self, *near):
        for piece in range(PIECES):
            for d in near:
                @pl.when(self.rank >= d)
                def _():
                    self.direct(d, piece).wait_recv()

                for make, other, used in self.routes()[3:]:
                    if other == d:
                        @pl.when(used)
                        def _():
                            make(d, piece).start()

    def stage(self, number):
        self.land(*((2, 4), (1,), (3,))[number])

    def drain(self):
        for make, d, used in self.routes():
            @pl.when(used)
            def _():
                for piece in range(PIECES):
                    make(d, piece).wait_send()


def braided(hops):
    return lax.axis_size("sub") == 2 and lax.axis_size("seq") % 2 == 0 and hops == 4


def halo(hops, *args):
    return (Braid if braided(hops) else Halo)(*args)


def halo_sems(hops, number):
    dma = pltpu.SemaphoreType.DMA
    if braided(hops):
        return [dma((number, 3, hops, PIECES)), dma((number, hops, PIECES))]
    return [dma((number, 2 * hops)), dma((number, hops))]


class Shift:
    def __init__(self, src, dst, send, recv, distance):
        me, count, subs = place()
        self.me, self.subs, self.target = me, subs, me + distance
        self.args = (src, dst, send, recv)
        self.sends = (me + distance >= 0) & (me + distance < count)
        self.gets = (me - distance >= 0) & (me - distance < count)
        self.copy = remote(src, dst, send, recv, jnp.clip(me + distance, 0, count - 1), subs)

    def start(self):
        @pl.when(self.sends)
        def _():
            self.copy.start()

    def wait(self):
        @pl.when(self.sends)
        def _():
            self.copy.wait_send()

        @pl.when(self.gets)
        def _():
            self.copy.wait_recv()


def window_masks(hops, rows, me):
    margin = hops * rows
    row = iota((2 * rows, rows), 0) % rows
    masks = []
    for b in range(hops + 1):
        least, most = margin - (b + 1) * rows + 1, margin + rows - 1 - b * rows
        gap = margin - b * rows + row - iota((2 * rows, rows), 1)
        mask = jnp.broadcast_to(me - (hops - b), gap.shape) >= 0
        if least < 0:
            mask = mask & (gap >= 0)
        if most >= WINDOW:
            mask = mask & (gap < WINDOW)
        masks.append(mask)
    return masks


def causal(keys, queries):
    return keys <= queries


class Coarse:
    def __init__(self, total, span, base, cw, cow, scratch):
        self.total, self.span, self.base = total, span, base
        self.cw, self.cow = cw, cow
        self.uq, self.fq, self.uk, self.fk, self.v, self.g = scratch
        self.width = cw.shape[2]

    def grads(self, cg):
        self.gb = dot_nt(cg, self.cow[...]).astype(BF16)
        self.g[pl.ds(0, self.total), :] = self.gb.astype(F32)

    def project(self, normed):
        uq, fq = head_rms(dot(normed, self.cw[0]))
        uk, fk = head_rms(dot(normed, self.cw[1]))
        v = dot(normed, self.cw[2])
        for ref, value in ((self.uq, uq), (self.fq, fq), (self.uk, uk), (self.fk, fk), (self.v, v)):
            ref[pl.ds(0, self.total), :] = value
        self.qb, self.kb, self.vb = (uq * QUERY).astype(BF16), uk.astype(BF16), v.astype(BF16)

    def sums(self, cols):
        block = min(self.total, 256)
        inverse, deltas = [], []
        for i in range(self.total // block):
            part = slice(i * block, (i + 1) * block)
            q, g = self.qb[part, cols], self.gb[part, cols]
            t, d = [0.0, 0.0], [0.0, 0.0]
            for j in range(i + 1):
                rows = slice(j * block, (j + 1) * block)
                e = jnp.exp2(dot_nt(both(self.kb[rows, cols]), q))
                if j == i:
                    e = jnp.where(causal(iota(e.shape, 0) % block, iota(e.shape, 1)), e, 0.0)
                ed = e * dot_nt(both(self.vb[rows, cols]), g)
                for h in range(2):
                    half = slice(h * block, (h + 1) * block)
                    t[h] = t[h] + jnp.sum(e[half], axis=0, keepdims=True)
                    d[h] = d[h] + jnp.sum(ed[half], axis=0, keepdims=True)
            inverse.append([1.0 / x for x in t])
            deltas.append([x * r for x, r in zip(d, inverse[-1])])
        join = lambda parts, h: jnp.concatenate([x[h] for x in parts], axis=1)
        return [join(inverse, h) for h in range(2)], [join(deltas, h) for h in range(2)]

    def mine(self, ref, cols):
        start = pl.multiple_of(self.base, 8)
        return ref[pl.ds(start, self.span), cols]

    def attend(self):
        span, total = self.span, self.total
        shape = (2 * span, total)
        own = self.base + iota(shape, 0) % span
        after = causal(own, iota(shape, 1))
        before = causal(iota(shape, 1), own)
        att_p, dq_p, dk_p, dv_p = [], [], [], []
        for p in range(self.width // PAIR):
            cols = slice(p * PAIR, (p + 1) * PAIR)
            inverse, deltas = self.sums(cols)
            ds_cols = pl.ds(p * PAIR, PAIR)
            qp, kp, vp, gp = self.qb[:, cols], self.kb[:, cols], self.vb[:, cols], self.gb[:, cols]
            k2, v2 = both(self.mine(self.uk, ds_cols)), both(self.mine(self.v, ds_cols))
            q2, g2 = both(self.mine(self.uq, ds_cols) * QUERY), both(self.mine(self.g, ds_cols))
            wide = lambda pair: jnp.concatenate([jnp.broadcast_to(x, (span, total)) for x in pair])
            pt = jnp.where(after, jnp.exp2(dot_nt(k2, qp)) * wide(inverse), 0.0)
            dst = pt * (dot_nt(v2, gp) - wide(deltas))
            dk_p.append(pick(dot(dst.astype(BF16), qp)) * LN2)
            dv_p.append(pick(dot(pt.astype(BF16), gp)))
            e = jnp.where(before, jnp.exp2(dot_nt(q2, kp)), 0.0)
            e = e * (1.0 / jnp.sum(e, axis=-1, keepdims=True))
            dp = dot_nt(g2, vp)
            delta = jnp.sum(e * dp, axis=-1, keepdims=True)
            ds = e * (dp - delta)
            dq_p.append(pick(dot(ds.astype(BF16), kp)) * SCALE)
            att_p.append(pick(dot(e.astype(BF16), vp)))
        join = lambda parts: jnp.concatenate(parts, axis=1)
        return join(att_p), join(dq_p), join(dk_p), join(dv_p)

    def finish(self, outs_all):
        every = pl.ds(0, self.width)
        att, dq, dk, dv = self.attend()
        mixed = dot(att[:outs_all].astype(BF16), self.cow[...])
        dq = head_back(dq, self.mine(self.uq, every), self.mine(self.fq, every)).astype(BF16)
        dk = head_back(dk, self.mine(self.uk, every), self.mine(self.fk, every)).astype(BF16)
        dv = dv.astype(BF16)
        return mixed, dot_nt(dq, self.cw[0]) + dot_nt(dk, self.cw[1]) + dot_nt(dv, self.cw[2])


def layer_pair(
    hops, x_hbm, cot_hbm, w_hbm, out_hbm, cw_hbm, cow_hbm, output_ref, grad_ref,
    x_ref, cot_ref,
    w_ref, out_w, cw, cow, before, q_all, cot_after, k_all, v_all,
    unit_q, unit_k, scale_q, scale_k, e_ref, t_ref, acc_ref, rt_ref, att_ref, hidden_ref,
    cg_own, cg_all, pool_own, pool_all, pooled, gcot, g_all,
    uq2, fq2, uk2, fk2, v2, g2, mixed_ref, ng_ref, x_out, x_in, stats, stats_after, dq_ref,
    load, halo_sends, halo_recvs, x_sems, stat_sems, *sems,
):
    me, count, subs = place()
    mine, seq = lax.axis_index("sub"), lax.axis_index("seq")
    rows = x_ref.shape[0]
    outs = rows // POOL
    margin, length = hops * rows, (hops + 1) * rows
    total = count * outs
    far = (hops + 2) * outs
    greet_all()
    parts = [
        (w_hbm.at[1], w_ref.at[1]), (w_hbm.at[2], w_ref.at[2]), (w_hbm.at[0], w_ref.at[0]),
        (out_hbm, out_w), (cw_hbm, cw), (cow_hbm, cow), (x_hbm, x_ref), (cot_hbm, cot_ref),
    ]
    loads = [pltpu.make_async_copy(src, dst, load.at[i]) for i, (src, dst) in enumerate(parts)]
    for one in loads[6:] + loads[:6]:
        one.start()
    for d in range(1, hops + 1):
        @pl.when(me - d < 0)
        def _():
            before[hops - d] = jnp.zeros((rows, D), BF16)

        @pl.when(me + d >= count)
        def _():
            q_all[d] = jnp.zeros((rows, D), BF16)
            cot_after[d - 1] = jnp.zeros((rows, D), BF16)
            stats_after[d - 1] = jnp.zeros(stats.shape, F32)

    extra = pooled.shape[0] - total
    pooled[pl.ds(total, extra), :] = jnp.zeros((extra, D), F32)
    cg_all[pl.ds(count, extra // outs)] = jnp.zeros((extra // outs, outs, D), BF16)
    for ref in (uq2, fq2, uk2, fk2, v2, g2):
        ref[pl.ds(total, extra), :] = jnp.zeros((extra, ref.shape[1]), F32)
    loads[6].wait()
    loads[7].wait()
    groups = (iota((outs, rows), 1) // POOL == iota((outs, rows), 0)).astype(F32).astype(BF16)
    cg_own[...] = dot(groups, cot_ref[...]).astype(BF16)
    own = x_ref[...].astype(F32)
    own_b = rms_rows(own)[0].astype(BF16)
    down = halo(hops, x_ref, before, halo_sends.at[0], halo_recvs.at[0], hops, 1)
    up_cot = halo(hops, cot_ref, cot_after, halo_sends.at[1], halo_recvs.at[1], hops, -1)
    up = halo(hops, q_all.at[0], q_all.at[pl.ds(1, hops)], halo_sends.at[2], halo_recvs.at[2], hops, -1)
    cg_spread = Spread(cg_own, cg_all, *sems[:4])
    pool_spread = Spread(pool_own, pool_all, *sems[4:])
    met_all()
    down.start()
    cg_spread.start()
    loads[0].wait()
    unit, factor = head_rms(dot(own_b, w_ref[1]))
    k_all[pl.ds(margin, rows), :] = unit.astype(BF16)
    unit_k[...] = unit
    scale_k[...] = factor
    loads[1].wait()
    v_all[pl.ds(margin, rows), :] = dot(own_b, w_ref[2]).astype(BF16)
    loads[2].wait()
    unit, factor = head_rms(dot(own_b, w_ref[0]))
    q_all[0] = (unit * QUERY).astype(BF16)
    unit_q[...] = unit
    scale_q[...] = factor

    def keys(d):
        slot = pl.ds(margin - d * rows, rows)
        prev = rms_rows(before[hops - d].astype(F32))[0].astype(BF16)
        k_all[slot, :] = head_rms(dot(prev, w_ref[1]))[0].astype(BF16)
        v_all[slot, :] = dot(prev, w_ref[2]).astype(BF16)

    masks = window_masks(hops, rows, me)

    def scores(p, blocks):
        low, high = blocks[0], blocks[-1] + 1
        cols = pl.ds(p * PAIR, PAIR)
        span = pl.ds(low * rows, (high - low) * rows)
        s = dot_nt(both(q_all[0, :, cols]), k_all[span, cols])
        e = [
            jnp.where(masks[b], jnp.exp2(s[:, (b - low) * rows : (b - low + 1) * rows]), 0.0)
            for b in range(low, high)
        ]
        e_b = jnp.concatenate(e, axis=1).astype(BF16)
        e_ref[p, :, span] = e_b
        return functools.reduce(jnp.add, e), dot(e_b, v_all[span, cols])

    half = hops // 2
    if braided(hops):
        for p in range(HEADS // 2):
            t_ref[p], acc_ref[p] = scores(p, [hops])
        down.land(2, 4)
        keys(2)
        keys(4)
        down.land(1)
        keys(1)
        cg_spread.widen()
        down.land(3)
        up_cot.start()
        keys(3)
        late = range(0, hops)
    else:
        for d in range(1, hops - half + 1):
            down.land(d)
            keys(d)
        cg_spread.widen()
        for p in range(HEADS // 2):
            t_ref[p], acc_ref[p] = scores(p, range(half, hops + 1))
        for d in range(hops - half + 1, hops + 1):
            down.land(d)
            keys(d)
        late = range(0, half)
        up_cot.start()
    cg_spread.cross()
    lane = iota((rows, 128), 1)
    totals = jnp.ones((rows, 128), F32)
    for p in range(HEADS // 2):
        t, acc = scores(p, late)
        t = jnp.sum(t + t_ref[p], axis=-1, keepdims=True)
        inverse = jnp.broadcast_to(1.0 / t, (2 * rows, PAIR))
        rt_ref[p] = inverse
        att_ref[:, pl.ds(p * PAIR, PAIR)] = pick((acc + acc_ref[p]) * inverse).astype(BF16)
        totals = jnp.where(lane == 2 * p, t[:rows], totals)
        totals = jnp.where(lane == 2 * p + 1, t[rows:], totals)
    loads[3].wait()
    hidden = (own + dot(att_ref[...], out_w[...])).astype(BF16)
    hidden_ref[...] = hidden
    back = iota((outs, rows), 0) * POOL - iota((outs, rows), 1)
    part = dot(((back >= 0) & (back < POOL)).astype(F32).astype(BF16), hidden)
    tail = dot((iota((outs, rows), 1) > rows - POOL).astype(F32).astype(BF16), hidden)
    lanes = D // outs
    folded = jnp.zeros((outs, lanes), F32)
    for c in range(outs):
        folded = jnp.where(iota((outs, lanes), 0) == c, tail[:, c * lanes : (c + 1) * lanes], folded)
    pool_own[...] = (jnp.concatenate([part, folded], axis=1) / POOL).astype(BF16)
    pool_spread.start()
    cg_spread.finish()
    loads[4].wait()
    loads[5].wait()
    base = seq * subs * outs
    span = (subs - 1) * outs + far
    coarse = Coarse(total, span, base, cw, cow, (uq2, fq2, uk2, fk2, v2, g2))
    coarse.grads(cg_all[pl.ds(0, count)].astype(F32).reshape(total, D).astype(BF16))
    gcot[...] = dot_nt(cot_ref[...], out_w[...])
    stats[pl.ds(0, HEADS), :] = jnp.log2(totals.T[:HEADS])
    pool_spread.widen()
    pool_spread.cross()
    pool_spread.finish()
    up_cot.stage(0)
    up.start()
    got = pool_all[...].astype(F32).reshape(total, D + lanes)
    block = min(total, 256)
    place_at = (iota((block, block), 0) // outs == iota((block, block), 1) // outs) & (iota((block, block), 0) % outs == 0)
    place_at = place_at.astype(F32).astype(BF16)
    tails = []
    for i in range(total // block):
        one = got[i * block : (i + 1) * block, D:]
        wide = [jnp.where(iota(one.shape, 0) % outs == c, one, 0.0) for c in range(outs)]
        tails.append(dot(place_at, jnp.concatenate(wide, axis=1).astype(BF16)))
    tails = jnp.concatenate([jnp.zeros((outs, D), F32)] + tails)[:total]
    pooled_v = (got[:, :D] + tails).astype(BF16).astype(F32)
    pooled[pl.ds(0, total), :] = pooled_v
    coarse.project(rms_rows(pooled_v)[0].astype(BF16))
    mixed, ng = coarse.finish(subs * outs)
    mixed_ref[...] = mixed
    ng_ref[...] = ng

    def cut(sub):
        start = pl.multiple_of(sub * outs, outs)
        return mixed_ref[pl.ds(start, outs), :], ng_ref[pl.ds(start, far), :]

    copies = []
    for k in range(1, subs):
        other = (mine + k) % subs
        x_out[k] = jnp.concatenate(cut(other)).astype(BF16)
        copies.append(remote(
            x_out.at[k], x_in.at[k], x_sems.at[0, k], x_sems.at[1, k], seq * subs + other, subs
        ))
        copies[-1].start()
    up_cot.stage(1)
    up.stage(0)
    mixed, ng = cut(mine)
    start = pl.multiple_of(me * outs, outs)
    pooled_own = pooled[pl.ds(start, far), :]
    cg = cg_all[pl.ds(me, far // outs)].astype(F32).reshape(far, D)
    normed, factor = rms_rows(pooled_own)
    for copy in copies:
        copy.wait()
    for k in range(1, subs):
        other = x_in[k].astype(F32)
        mixed, ng = mixed + other[:outs], ng + other[outs:]
    pg = (cg + row_back(ng, normed, factor)) / POOL
    pg = jnp.where(me * outs + iota(pg.shape, 0) < total, pg, 0.0).astype(BF16)
    pgw = dot_nt(pg, out_w[...]).astype(BF16)
    lift = ((iota((length, far), 0) + POOL - 1) // POOL == iota((length, far), 1)).astype(F32).astype(BF16)
    g_all[pl.ds(0, rows), :] = (gcot[...] + dot(lift[:rows], pgw)).astype(BF16)
    delta = head_sum(g_all[pl.ds(0, rows), :].astype(F32) * att_ref[...].astype(F32))
    stats[pl.ds(HEADS, HEADS), :] = delta.T[:HEADS]
    moves = [
        Shift(stats, stats_after.at[d - 1], stat_sems.at[0, d - 1], stat_sems.at[1, d - 1], -d)
        for d in range(1, hops + 1)
    ]
    for move in moves:
        move.start()
    up.stage(1)
    state = (pooled_own[:outs] + mixed).astype(BF16)
    onto = (iota((rows, outs), 0) // POOL == iota((rows, outs), 1)).astype(F32).astype(BF16)
    output_ref[...] = (hidden_ref[...].astype(F32) + dot(onto, state)).astype(BF16)
    for p in range(HEADS // 2):
        cols = pl.ds(p * PAIR, PAIR)
        dp = dot_nt(both(g_all[pl.ds(0, rows), cols]), v_all[:, cols])
        column = jnp.concatenate([delta[:, 2 * p : 2 * p + 1], delta[:, 2 * p + 1 : 2 * p + 2]])
        ds = (e_ref[p].astype(F32) * (dp - column)).astype(BF16)
        dq_ref[:, cols] = pick(dot(ds, k_all[:, cols]) * rt_ref[p]) * SCALE
    dq = head_back(dq_ref[...], unit_q[...], scale_q[...]).astype(BF16)
    dq_ref[...] = dot_nt(dq, w_ref[0])
    up_cot.stage(2)
    later = dot_nt(cot_after[...].reshape(margin, D), out_w[...])
    g_all[pl.ds(rows, margin), :] = (later + dot(lift[rows:], pgw)).astype(BF16)
    up.stage(2)
    for move in moves:
        move.wait()
    gap = iota((rows, length), 1) - iota((rows, length), 0)
    mask_t = (gap >= 0) & (gap < WINDOW)
    every = jnp.concatenate([stats[...]] + [stats_after[d] for d in range(hops)], axis=1)
    dk_p, dv_p = [], []
    for p in range(HEADS // 2):
        cols = pl.ds(p * PAIR, PAIR)
        own_slot = pl.ds(margin, rows)
        qp, gp = q_all[:, :, cols].reshape(length, PAIR), g_all[:, cols]
        st = dot_nt(both(k_all[own_slot, cols]), qp)
        dpt = dot_nt(both(v_all[own_slot, cols]), gp)
        pts, dsts = [], []
        for h in range(2):
            head = 2 * p + h
            part = slice(h * rows, (h + 1) * rows)
            pt = jnp.where(mask_t, jnp.exp2(st[part] - every[head : head + 1]), 0.0)
            pts.append(pt.astype(BF16))
            dsts.append((pt * (dpt[part] - every[HEADS + head : HEADS + head + 1])).astype(BF16))
        dk_p.append(pick(dot(jnp.concatenate(dsts), qp)) * LN2)
        dv_p.append(pick(dot(jnp.concatenate(pts), gp)))
    join = lambda parts: jnp.concatenate(parts, axis=1)
    dk = head_back(join(dk_p), unit_k[...], scale_k[...]).astype(BF16)
    dv = join(dv_p).astype(BF16)
    grads = dq_ref[...] + dot_nt(dk, w_ref[1]) + dot_nt(dv, w_ref[2])
    normed, factor = rms_rows(x_ref[...].astype(F32))
    hidden_grad = cot_ref[...].astype(F32) + dot(lift[:rows], pg)
    grad_ref[...] = (hidden_grad + row_back(grads, normed, factor)).astype(BF16)
    down.drain()
    up_cot.drain()
    up.drain()


def per_device(tokens, cotangent, fine_qkv, fine_out, coarse_qkv, coarse_out):
    rows = tokens.shape[0]
    hops = -(-WINDOW // rows)
    outs = rows // POOL
    me, count, subs = place()
    far = (hops + 2) * outs
    length = (hops + 1) * rows
    total = count * outs
    span = (subs - 1) * outs + far
    width = coarse_qkv.shape[2]
    pairs = HEADS // 2
    shape = jax.ShapeDtypeStruct
    dma = pltpu.SemaphoreType.DMA
    vmem = pltpu.VMEM
    fine_w = jnp.transpose(fine_qkv, (1, 0, 2))
    coarse_w = jnp.transpose(coarse_qkv, (1, 0, 2))
    wide = D + D // outs
    padded = total + far
    scratch = [
        vmem((rows, D), BF16), vmem((rows, D), BF16),
        vmem(fine_w.shape, BF16), vmem(fine_out.shape, BF16), vmem(coarse_w.shape, BF16),
        vmem(coarse_out.shape, BF16),
        vmem((hops, rows, D), BF16), vmem((hops + 1, rows, D), BF16), vmem((hops, rows, D), BF16),
        vmem((length, D), BF16), vmem((length, D), BF16),
        vmem((rows, D), F32), vmem((rows, D), F32), vmem((rows, D), F32), vmem((rows, D), F32),
        vmem((pairs, 2 * rows, length), BF16), vmem((pairs, 2 * rows, rows), F32),
        vmem((pairs, 2 * rows, PAIR), F32), vmem((pairs, 2 * rows, PAIR), F32),
        vmem((rows, D), BF16), vmem((rows, D), BF16),
        vmem((outs, D), BF16), vmem((count + far // outs, outs, D), BF16),
        vmem((outs, wide), BF16), vmem((count, outs, wide), BF16),
        vmem((padded, D), F32), vmem((rows, D), F32), vmem((length, D), BF16),
    ] + [vmem((padded, width), F32)] * 6 + [
        vmem((subs * outs, D), F32), vmem((span, D), F32),
        vmem((subs, outs + far, D), BF16), vmem((subs, outs + far, D), BF16),
        vmem((2 * HEADS, rows), F32), vmem((hops, 2 * HEADS, rows), F32), vmem((rows, D), F32),
        dma((8,)), *halo_sems(hops, 3), dma((2, subs)), dma((2, hops)),
    ] + spread_sems(count, subs) * 2
    return pl.pallas_call(
        functools.partial(layer_pair, hops),
        out_shape=[shape((rows, D), BF16)] * 2,
        in_specs=[HBM] * 6,
        out_specs=[VMEM] * 2,
        scratch_shapes=scratch,
        compiler_params=pltpu.CompilerParams(
            collective_id=0, has_side_effects=True, vmem_limit_bytes=(48 if total <= 1024 else 63) * 1024 * 1024
        ),
    )(*[
        pltpu.with_memory_space_constraint(a, pltpu.HBM)
        for a in (tokens, cotangent, fine_w, fine_out, coarse_w, coarse_out)
    ])


def solution(mesh):
    placed = (
        P(("seq", "sub"), None),
        P(("seq", "sub"), None),
        P(),
        P(),
        P(None, None, "sub"),
        P("sub", None),
    )
    return jax.shard_map(
        per_device,
        mesh=mesh,
        in_specs=placed,
        out_specs=(P(("seq", "sub"), None), P(("seq", "sub"), None)),
        check_vma=False,
    )
```

```python
import functools
import math

import jax
import jax.numpy as jnp
from jax import lax
from jax.experimental import pallas as pl
from jax.experimental.pallas import tpu as pltpu
from jax.sharding import PartitionSpec as P

D = 1024
HEADS = 16
HEAD_DIM = 64
WINDOW = 512
POOL = 16
PIECES = 2
EPS = 1e-06
F32 = jnp.float32
BF16 = jnp.bfloat16
MESH = pl.DeviceIdType.MESH
PAIR = 2 * HEAD_DIM
SCALE = HEAD_DIM ** (-0.5)
LN2 = math.log(2.0)
QUERY = SCALE / LN2
VMEM = pl.BlockSpec(memory_space=pltpu.VMEM)
HBM = pl.BlockSpec(memory_space=pltpu.HBM)
SMEM = pl.BlockSpec(memory_space=pltpu.SMEM)


def dot(a, b):
    return jnp.dot(a, b, preferred_element_type=F32)


def dot_nt(a, b):
    return lax.dot_general(a, b, (((1,), (1,)), ((), ())), preferred_element_type=F32)


def dot_tn(a, b):
    return lax.dot_general(a, b, (((0,), (0,)), ((), ())), preferred_element_type=F32)


def split(x):
    hi = x.astype(BF16)
    return hi, (x - hi.astype(F32)).astype(BF16)


def iota(shape, axis):
    return lax.broadcasted_iota(jnp.int32, shape, axis)


def head_sum(x):
    group = (iota((x.shape[1], 128), 0) // HEAD_DIM == iota((x.shape[1], 128), 1)).astype(F32).astype(BF16)
    hi, lo = split(x)
    return dot(hi, group) + dot(lo, group)


def head_mean(x):
    group = iota((PAIR, PAIR), 0) // HEAD_DIM == iota((PAIR, PAIR), 1) // HEAD_DIM
    group = jnp.where(group, 1.0 / HEAD_DIM, 0.0).astype(BF16)
    x = x.astype(BF16)
    return jnp.concatenate([dot(x[:, c : c + PAIR], group) for c in range(0, x.shape[1], PAIR)], axis=1)


def head_rms(raw):
    factor = lax.rsqrt(head_mean(raw * raw) + EPS)
    return raw * factor, factor


def head_back(grad, unit, factor):
    return factor * (grad - unit * head_mean(unit * grad))


def rms_rows(x):
    factor = lax.rsqrt(jnp.mean(x * x, axis=-1, keepdims=True) + EPS)
    return x * factor, factor


def row_back(grad, normed, factor):
    return factor * (grad - normed * jnp.mean(normed * grad, axis=-1, keepdims=True))


def both(pair):
    low = iota(pair.shape, 1) < HEAD_DIM
    wide = pair.astype(F32)
    return jnp.concatenate([jnp.where(low, wide, 0.0), jnp.where(low, 0.0, wide)]).astype(BF16)


def pick(stacked):
    half = stacked.shape[0] // 2
    low = iota((half, PAIR), 1) < HEAD_DIM
    return jnp.where(low, stacked[:half], stacked[half:])


def place():
    subs = lax.axis_size("sub")
    count = lax.axis_size("seq") * subs
    me = lax.axis_index("seq") * subs + lax.axis_index("sub")
    return me, count, subs


def coords(index, subs):
    return (index // subs, index % subs)


def greet_all():
    me, count, subs = place()
    barrier = pltpu.get_barrier_semaphore()

    @pl.loop(1, count)
    def _(k):
        pl.semaphore_signal(
            barrier, inc=1, device_id=coords((me + k) % count, subs), device_id_type=MESH
        )


def met_all():
    pl.semaphore_wait(pltpu.get_barrier_semaphore(), lax.axis_size("seq") * lax.axis_size("sub") - 1)


def remote(src, dst, send, recv, target, subs):
    return pltpu.make_async_remote_copy(
        src_ref=src, dst_ref=dst, send_sem=send, recv_sem=recv,
        device_id=coords(target, subs), device_id_type=MESH,
    )


class Spread:
    def __init__(self, src, dst, out_sem, mid_sem, last_sem, sent):
        self.me, self.count, self.subs = place()
        self.cores = 2 if lax.axis_size("seq") % 2 == 0 else 1
        self.groups = self.count // self.subs // self.cores
        self.sub = self.me % self.subs
        self.core = self.me // self.subs % self.cores
        self.group = self.me // self.subs // self.cores
        self.src, self.dst, self.sems, self.sent = src, dst, (out_sem, mid_sem, last_sem), sent

    def index(self, k, core, j):
        group = (self.group + self.groups - k) % self.groups
        sub = (self.sub + self.subs - j) % self.subs
        return (group * self.cores + (self.core + core) % self.cores) * self.subs + sub

    def copy(self, phase, j, k):
        if phase == 0:
            spot, source = self.me, self.src
            target, sem = self.index(self.groups - k, 0, 0), self.sems[0].at[k]
        elif phase == 1:
            spot = self.index(k, 0, 0)
            target, sem = self.index(0, 0, self.subs - j), self.sems[1].at[j, k]
        else:
            spot = self.index(k, 0, j)
            target, sem = self.index(0, 1, 0), self.sems[2].at[j, k]
        source = self.src if phase == 0 else self.dst.at[spot]
        return remote(source, self.dst.at[spot], self.sent.at[phase, j, k], sem, target, self.subs)

    def arrive(self, phase, j, k):
        if phase == 0:
            spot, sem = self.index(k, 0, 0), self.sems[0].at[k]
        elif phase == 1:
            spot, sem = self.index(k, 0, j), self.sems[1].at[j, k]
        else:
            spot, sem = self.index(k, 1, j), self.sems[2].at[j, k]
        other = (self.me + 1) % self.count
        return remote(self.dst.at[spot], self.dst.at[spot], self.sent.at[phase, j, k], sem, other, self.subs)

    def relay(self, k):
        for j in range(1, self.subs):
            self.copy(1, j, k).start()
        if self.cores > 1:
            self.copy(2, 0, k).start()

    def start(self):
        self.dst[self.me] = self.src[...]

        @pl.loop(1, self.groups)
        def _(k):
            self.copy(0, 0, k).start()

        self.relay(0)

    def widen(self):
        @pl.loop(1, self.groups)
        def _(k):
            self.arrive(0, 0, k).wait_recv()
            self.relay(k)

    def cross(self):
        @pl.loop(0, self.groups)
        def _(k):
            for j in range(1, self.subs):
                self.arrive(1, j, k).wait_recv()
                if self.cores > 1:
                    self.copy(2, j, k).start()

    def finish(self):
        @pl.loop(0, self.groups)
        def _(k):
            for j in range(self.subs):
                if self.cores > 1:
                    self.arrive(2, j, k).wait_recv()
                    self.copy(2, j, k).wait_send()
                if j > 0:
                    self.copy(1, j, k).wait_send()

        @pl.loop(1, self.groups)
        def _(k):
            self.copy(0, 0, k).wait_send()


def spread_sems(count, subs):
    cores = 2 if count // subs % 2 == 0 else 1
    groups = count // subs // cores
    dma = pltpu.SemaphoreType.DMA
    return [dma((groups,)), dma((subs, groups)), dma((subs, groups)), dma((3, subs, groups))]


class Halo:
    def __init__(self, src, dst, sends, recvs, hops, sign):
        self.me, self.count, self.subs = place()
        self.src, self.dst, self.sends, self.recvs = src, dst, sends, recvs
        self.hops, self.sign = hops, sign
        self.paired = lax.axis_size("seq") % 2 == 0
        far_core = self.me // self.subs % 2
        self.first = far_core == (0 if sign > 0 else 1)

    def slot(self, d):
        return self.dst.at[self.hops - d if self.sign > 0 else d - 1]

    def inside(self, index):
        return (index >= 0) & (index < self.count)

    def cuts(self, d):
        if not self.paired or d <= self.subs:
            return self.inside(self.me + self.sign * d)
        target = self.me + self.sign * d + 2 * self.count * self.subs
        core = target // self.subs % 2
        return self.inside(self.me + self.sign * d) & (core == (0 if self.sign > 0 else 1))

    def direct(self, d):
        target = jnp.clip(self.me + self.sign * d, 0, self.count - 1)
        return remote(self.src, self.slot(d), self.sends.at[d - 1], self.recvs.at[d - 1], target, self.subs)

    def passed(self, d):
        target = jnp.clip(self.me + self.sign * self.subs, 0, self.count - 1)
        to = d + self.subs
        return remote(
            self.slot(d), self.slot(to), self.sends.at[self.hops + to - 1], self.recvs.at[to - 1],
            target, self.subs,
        )

    def relays(self, d):
        return self.first & self.inside(self.me - self.sign * d)

    def start(self):
        for d in range(1, self.hops + 1):
            @pl.when(self.cuts(d))
            def _():
                self.direct(d).start()

    def land(self, *near):
        for d in near:
            self.land_one(d)

    def land_one(self, d):
        @pl.when(self.inside(self.me - self.sign * d))
        def _():
            self.direct(d).wait_recv()

        if self.paired and d + self.subs <= self.hops:
            @pl.when(self.relays(d))
            def _():
                self.passed(d).start()

    def stage(self, number):
        if number == 0:
            self.land(*range(1, self.hops + 1))

    def drain(self):
        for d in range(1, self.hops + 1):
            @pl.when(self.cuts(d))
            def _():
                self.direct(d).wait_send()

            if self.paired and d + self.subs <= self.hops:
                @pl.when(self.relays(d))
                def _():
                    self.passed(d).wait_send()


class Braid:
    def __init__(self, src, dst, sends, recvs, hops, sign):
        self.me, self.count, self.subs = place()
        self.src, self.dst, self.sends, self.recvs = src, dst, sends, recvs
        self.hops, self.sign = hops, sign
        self.rank = self.me if sign > 0 else self.count - 1 - self.me
        self.side, self.core = self.rank % 2, self.rank // 2 % 2
        self.size = src.shape[0] // PIECES

    def slot(self, d):
        return self.dst.at[self.hops - d if self.sign > 0 else d - 1]

    def copy(self, kind, source, d, to, slot, piece):
        span = pl.ds(piece * self.size, self.size)
        target = jnp.clip(self.me + self.sign * to, 0, self.count - 1)
        return remote(
            source.at[span], self.slot(slot).at[span], self.sends.at[kind, d - 1, piece],
            self.recvs.at[slot - 1, piece], target, self.subs,
        )

    def direct(self, d, piece):
        return self.copy(0, self.src, d, d, d, piece)

    def across(self, d, piece):
        step = 1 - 2 * self.side
        return self.copy(1, self.slot(d), d, step, d + step, piece)

    def passed(self, d, piece):
        return self.copy(2, self.slot(d), d, 2, d + 2, piece)

    def routes(self):
        near = self.core == 0
        return [
            (self.direct, 2, self.rank + 2 < self.count),
            (self.direct, 4, near & (self.rank + 4 < self.count)),
            (self.direct, 1, (self.rank % 4 != 3) & (self.rank + 1 < self.count)),
            (self.across, 2, near & (self.rank >= 2)),
            (self.across, 4, near & (self.side == 1) & (self.rank >= 4)),
            (self.passed, 1, near & (self.rank >= 1)),
            (self.passed, 2, near & (self.rank >= 2)),
        ]

    def start(self):
        for make, d, used in self.routes()[:3]:
            @pl.when(used)
            def _():
                for piece in range(PIECES):
                    make(d, piece).start()

    def land(self, *near):
        for piece in range(PIECES):
            for d in near:
                @pl.when(self.rank >= d)
                def _():
                    self.direct(d, piece).wait_recv()

                for make, other, used in self.routes()[3:]:
                    if other == d:
                        @pl.when(used)
                        def _():
                            make(d, piece).start()

    def stage(self, number):
        self.land(*((2, 4), (1,), (3,))[number])

    def drain(self):
        for make, d, used in self.routes():
            @pl.when(used)
            def _():
                for piece in range(PIECES):
                    make(d, piece).wait_send()


def braided(hops):
    return lax.axis_size("sub") == 2 and lax.axis_size("seq") % 2 == 0 and hops == 4


def halo(hops, *args):
    return (Braid if braided(hops) else Halo)(*args)


def halo_sems(hops, number):
    dma = pltpu.SemaphoreType.DMA
    if braided(hops):
        return [dma((number, 3, hops, PIECES)), dma((number, hops, PIECES))]
    return [dma((number, 2 * hops)), dma((number, hops))]


class Shift:
    def __init__(self, src, dst, send, recv, distance):
        me, count, subs = place()
        self.me, self.subs, self.target = me, subs, me + distance
        self.args = (src, dst, send, recv)
        self.sends = (me + distance >= 0) & (me + distance < count)
        self.gets = (me - distance >= 0) & (me - distance < count)
        self.copy = remote(src, dst, send, recv, jnp.clip(me + distance, 0, count - 1), subs)

    def start(self):
        @pl.when(self.sends)
        def _():
            self.copy.start()

    def wait(self):
        @pl.when(self.sends)
        def _():
            self.copy.wait_send()

        @pl.when(self.gets)
        def _():
            self.copy.wait_recv()


def window_masks(hops, rows, me):
    margin = hops * rows
    row = iota((2 * rows, rows), 0) % rows
    masks = []
    for b in range(hops + 1):
        least, most = margin - (b + 1) * rows + 1, margin + rows - 1 - b * rows
        gap = margin - b * rows + row - iota((2 * rows, rows), 1)
        mask = jnp.broadcast_to(me - (hops - b), gap.shape) >= 0
        if least < 0:
            mask = mask & (gap >= 0)
        if most >= WINDOW:
            mask = mask & (gap < WINDOW)
        masks.append(mask)
    return masks


def causal(keys, queries):
    return keys <= queries


class Coarse:
    def __init__(self, total, span, base, cw, cow, scratch):
        self.total, self.span, self.base = total, span, base
        self.cw, self.cow = cw, cow
        self.uq, self.fq, self.uk, self.fk, self.v, self.g = scratch
        self.width = cw.shape[2]

    def grads(self, cg):
        self.gb = dot_nt(cg, self.cow[...]).astype(BF16)
        self.g[pl.ds(0, self.total), :] = self.gb.astype(F32)

    def project(self, normed):
        uq, fq = head_rms(dot(normed, self.cw[0]))
        uk, fk = head_rms(dot(normed, self.cw[1]))
        v = dot(normed, self.cw[2])
        for ref, value in ((self.uq, uq), (self.fq, fq), (self.uk, uk), (self.fk, fk), (self.v, v)):
            ref[pl.ds(0, self.total), :] = value
        self.qb, self.kb, self.vb = (uq * QUERY).astype(BF16), uk.astype(BF16), v.astype(BF16)

    def sums(self, cols):
        block = min(self.total, 256)
        inverse, deltas = [], []
        for i in range(self.total // block):
            part = slice(i * block, (i + 1) * block)
            q, g = self.qb[part, cols], self.gb[part, cols]
            t, d = [0.0, 0.0], [0.0, 0.0]
            for j in range(i + 1):
                rows = slice(j * block, (j + 1) * block)
                e = jnp.exp2(dot_nt(both(self.kb[rows, cols]), q))
                if j == i:
                    e = jnp.where(causal(iota(e.shape, 0) % block, iota(e.shape, 1)), e, 0.0)
                ed = e * dot_nt(both(self.vb[rows, cols]), g)
                for h in range(2):
                    half = slice(h * block, (h + 1) * block)
                    t[h] = t[h] + jnp.sum(e[half], axis=0, keepdims=True)
                    d[h] = d[h] + jnp.sum(ed[half], axis=0, keepdims=True)
            inverse.append([1.0 / x for x in t])
            deltas.append([x * r for x, r in zip(d, inverse[-1])])
        join = lambda parts, h: jnp.concatenate([x[h] for x in parts], axis=1)
        return [join(inverse, h) for h in range(2)], [join(deltas, h) for h in range(2)]

    def mine(self, ref, cols):
        start = pl.multiple_of(self.base, 8)
        return ref[pl.ds(start, self.span), cols]

    def attend(self):
        span, total = self.span, self.total
        shape = (2 * span, total)
        own = self.base + iota(shape, 0) % span
        after = causal(own, iota(shape, 1))
        before = causal(iota(shape, 1), own)
        att_p, dq_p, dk_p, dv_p = [], [], [], []
        for p in range(self.width // PAIR):
            cols = slice(p * PAIR, (p + 1) * PAIR)
            inverse, deltas = self.sums(cols)
            ds_cols = pl.ds(p * PAIR, PAIR)
            qp, kp, vp, gp = self.qb[:, cols], self.kb[:, cols], self.vb[:, cols], self.gb[:, cols]
            k2, v2 = both(self.mine(self.uk, ds_cols)), both(self.mine(self.v, ds_cols))
            q2, g2 = both(self.mine(self.uq, ds_cols) * QUERY), both(self.mine(self.g, ds_cols))
            wide = lambda pair: jnp.concatenate([jnp.broadcast_to(x, (span, total)) for x in pair])
            pt = jnp.where(after, jnp.exp2(dot_nt(k2, qp)) * wide(inverse), 0.0)
            dst = pt * (dot_nt(v2, gp) - wide(deltas))
            dk_p.append(pick(dot(dst.astype(BF16), qp)) * LN2)
            dv_p.append(pick(dot(pt.astype(BF16), gp)))
            e = jnp.where(before, jnp.exp2(dot_nt(q2, kp)), 0.0)
            e = e * (1.0 / jnp.sum(e, axis=-1, keepdims=True))
            dp = dot_nt(g2, vp)
            delta = jnp.sum(e * dp, axis=-1, keepdims=True)
            ds = e * (dp - delta)
            dq_p.append(pick(dot(ds.astype(BF16), kp)) * SCALE)
            att_p.append(pick(dot(e.astype(BF16), vp)))
        join = lambda parts: jnp.concatenate(parts, axis=1)
        return join(att_p), join(dq_p), join(dk_p), join(dv_p)

    def finish(self, outs_all):
        every = pl.ds(0, self.width)
        att, dq, dk, dv = self.attend()
        mixed = dot(att[:outs_all].astype(BF16), self.cow[...])
        dq = head_back(dq, self.mine(self.uq, every), self.mine(self.fq, every)).astype(BF16)
        dk = head_back(dk, self.mine(self.uk, every), self.mine(self.fk, every)).astype(BF16)
        dv = dv.astype(BF16)
        return mixed, dot_nt(dq, self.cw[0]) + dot_nt(dk, self.cw[1]) + dot_nt(dv, self.cw[2])


def layer_pair(
    hops, x_hbm, cot_hbm, w_hbm, out_hbm, cw_hbm, cow_hbm, output_ref, grad_ref,
    x_ref, cot_ref,
    w_ref, out_w, cw, cow, before, q_all, cot_after, k_all, v_all,
    unit_q, unit_k, scale_q, scale_k, e_ref, t_ref, acc_ref, rt_ref, att_ref, hidden_ref,
    cg_own, cg_all, pool_own, pool_all, pooled, gcot, g_all,
    uq2, fq2, uk2, fk2, v2, g2, mixed_ref, ng_ref, x_out, x_in, stats, stats_after, dq_ref,
    load, halo_sends, halo_recvs, x_sems, stat_sems, *sems,
):
    me, count, subs = place()
    mine, seq = lax.axis_index("sub"), lax.axis_index("seq")
    rows = x_ref.shape[0]
    outs = rows // POOL
    margin, length = hops * rows, (hops + 1) * rows
    total = count * outs
    far = (hops + 2) * outs
    greet_all()
    parts = [
        (w_hbm.at[1], w_ref.at[1]), (w_hbm.at[2], w_ref.at[2]), (w_hbm.at[0], w_ref.at[0]),
        (out_hbm, out_w), (cw_hbm, cw), (cow_hbm, cow), (x_hbm, x_ref), (cot_hbm, cot_ref),
    ]
    loads = [pltpu.make_async_copy(src, dst, load.at[i]) for i, (src, dst) in enumerate(parts)]
    for one in loads[6:] + loads[:6]:
        one.start()
    for d in range(1, hops + 1):
        @pl.when(me - d < 0)
        def _():
            before[hops - d] = jnp.zeros((rows, D), BF16)

        @pl.when(me + d >= count)
        def _():
            q_all[d] = jnp.zeros((rows, D), BF16)
            cot_after[d - 1] = jnp.zeros((rows, D), BF16)
            stats_after[d - 1] = jnp.zeros(stats.shape, F32)

    extra = pooled.shape[0] - total
    pooled[pl.ds(total, extra), :] = jnp.zeros((extra, D), F32)
    cg_all[pl.ds(count, extra // outs)] = jnp.zeros((extra // outs, outs, D), BF16)
    for ref in (uq2, fq2, uk2, fk2, v2, g2):
        ref[pl.ds(total, extra), :] = jnp.zeros((extra, ref.shape[1]), F32)
    loads[6].wait()
    loads[7].wait()
    groups = (iota((outs, rows), 1) // POOL == iota((outs, rows), 0)).astype(F32).astype(BF16)
    cg_own[...] = dot(groups, cot_ref[...]).astype(BF16)
    own = x_ref[...].astype(F32)
    own_b = rms_rows(own)[0].astype(BF16)
    down = halo(hops, x_ref, before, halo_sends.at[0], halo_recvs.at[0], hops, 1)
    up_cot = halo(hops, cot_ref, cot_after, halo_sends.at[1], halo_recvs.at[1], hops, -1)
    up = halo(hops, q_all.at[0], q_all.at[pl.ds(1, hops)], halo_sends.at[2], halo_recvs.at[2], hops, -1)
    cg_spread = Spread(cg_own, cg_all, *sems[:4])
    pool_spread = Spread(pool_own, pool_all, *sems[4:])
    met_all()
    down.start()
    cg_spread.start()
    loads[0].wait()
    unit, factor = head_rms(dot(own_b, w_ref[1]))
    k_all[pl.ds(margin, rows), :] = unit.astype(BF16)
    unit_k[...] = unit
    scale_k[...] = factor
    loads[1].wait()
    v_all[pl.ds(margin, rows), :] = dot(own_b, w_ref[2]).astype(BF16)
    loads[2].wait()
    unit, factor = head_rms(dot(own_b, w_ref[0]))
    q_all[0] = (unit * QUERY).astype(BF16)
    unit_q[...] = unit
    scale_q[...] = factor

    def keys(d):
        slot = pl.ds(margin - d * rows, rows)
        prev = rms_rows(before[hops - d].astype(F32))[0].astype(BF16)
        k_all[slot, :] = head_rms(dot(prev, w_ref[1]))[0].astype(BF16)
        v_all[slot, :] = dot(prev, w_ref[2]).astype(BF16)

    masks = window_masks(hops, rows, me)

    def scores(p, blocks):
        low, high = blocks[0], blocks[-1] + 1
        cols = pl.ds(p * PAIR, PAIR)
        span = pl.ds(low * rows, (high - low) * rows)
        s = dot_nt(both(q_all[0, :, cols]), k_all[span, cols])
        e = [
            jnp.where(masks[b], jnp.exp2(s[:, (b - low) * rows : (b - low + 1) * rows]), 0.0)
            for b in range(low, high)
        ]
        e_b = jnp.concatenate(e, axis=1).astype(BF16)
        e_ref[p, :, span] = e_b
        return functools.reduce(jnp.add, e), dot(e_b, v_all[span, cols])

    half = hops // 2
    if braided(hops):
        for p in range(HEADS // 2):
            t_ref[p], acc_ref[p] = scores(p, [hops])
        down.land(2, 4)
        keys(2)
        keys(4)
        down.land(1)
        keys(1)
        cg_spread.widen()
        down.land(3)
        up_cot.start()
        keys(3)
        late = range(0, hops)
    else:
        for d in range(1, hops - half + 1):
            down.land(d)
            keys(d)
        cg_spread.widen()
        for p in range(HEADS // 2):
            t_ref[p], acc_ref[p] = scores(p, range(half, hops + 1))
        for d in range(hops - half + 1, hops + 1):
            down.land(d)
            keys(d)
        late = range(0, half)
        up_cot.start()
    cg_spread.cross()
    lane = iota((rows, 128), 1)
    totals = jnp.ones((rows, 128), F32)
    for p in range(HEADS // 2):
        t, acc = scores(p, late)
        t = jnp.sum(t + t_ref[p], axis=-1, keepdims=True)
        inverse = jnp.broadcast_to(1.0 / t, (2 * rows, PAIR))
        rt_ref[p] = inverse
        att_ref[:, pl.ds(p * PAIR, PAIR)] = pick((acc + acc_ref[p]) * inverse).astype(BF16)
        totals = jnp.where(lane == 2 * p, t[:rows], totals)
        totals = jnp.where(lane == 2 * p + 1, t[rows:], totals)
    loads[3].wait()
    hidden = (own + dot(att_ref[...], out_w[...])).astype(BF16)
    hidden_ref[...] = hidden
    back = iota((outs, rows), 0) * POOL - iota((outs, rows), 1)
    part = dot(((back >= 0) & (back < POOL)).astype(F32).astype(BF16), hidden)
    tail = dot((iota((outs, rows), 1) > rows - POOL).astype(F32).astype(BF16), hidden)
    lanes = D // outs
    folded = jnp.zeros((outs, lanes), F32)
    for c in range(outs):
        folded = jnp.where(iota((outs, lanes), 0) == c, tail[:, c * lanes : (c + 1) * lanes], folded)
    pool_own[...] = (jnp.concatenate([part, folded], axis=1) / POOL).astype(BF16)
    pool_spread.start()
    cg_spread.finish()
    loads[4].wait()
    loads[5].wait()
    base = seq * subs * outs
    span = (subs - 1) * outs + far
    coarse = Coarse(total, span, base, cw, cow, (uq2, fq2, uk2, fk2, v2, g2))
    coarse.grads(cg_all[pl.ds(0, count)].astype(F32).reshape(total, D).astype(BF16))
    gcot[...] = dot_nt(cot_ref[...], out_w[...])
    stats[pl.ds(0, HEADS), :] = jnp.log2(totals.T[:HEADS])
    pool_spread.widen()
    pool_spread.cross()
    pool_spread.finish()
    up_cot.stage(0)
    up.start()
    got = pool_all[...].astype(F32).reshape(total, D + lanes)
    block = min(total, 256)
    place_at = (iota((block, block), 0) // outs == iota((block, block), 1) // outs) & (iota((block, block), 0) % outs == 0)
    place_at = place_at.astype(F32).astype(BF16)
    tails = []
    for i in range(total // block):
        one = got[i * block : (i + 1) * block, D:]
        wide = [jnp.where(iota(one.shape, 0) % outs == c, one, 0.0) for c in range(outs)]
        tails.append(dot(place_at, jnp.concatenate(wide, axis=1).astype(BF16)))
    tails = jnp.concatenate([jnp.zeros((outs, D), F32)] + tails)[:total]
    pooled_v = (got[:, :D] + tails).astype(BF16).astype(F32)
    pooled[pl.ds(0, total), :] = pooled_v
    coarse.project(rms_rows(pooled_v)[0].astype(BF16))
    mixed, ng = coarse.finish(subs * outs)
    mixed_ref[...] = mixed
    ng_ref[...] = ng

    def cut(sub):
        start = pl.multiple_of(sub * outs, outs)
        return mixed_ref[pl.ds(start, outs), :], ng_ref[pl.ds(start, far), :]

    copies = []
    for k in range(1, subs):
        other = (mine + k) % subs
        x_out[k] = jnp.concatenate(cut(other)).astype(BF16)
        copies.append(remote(
            x_out.at[k], x_in.at[k], x_sems.at[0, k], x_sems.at[1, k], seq * subs + other, subs
        ))
        copies[-1].start()
    up_cot.stage(1)
    up.stage(0)
    mixed, ng = cut(mine)
    start = pl.multiple_of(me * outs, outs)
    pooled_own = pooled[pl.ds(start, far), :]
    cg = cg_all[pl.ds(me, far // outs)].astype(F32).reshape(far, D)
    normed, factor = rms_rows(pooled_own)
    for copy in copies:
        copy.wait()
    for k in range(1, subs):
        other = x_in[k].astype(F32)
        mixed, ng = mixed + other[:outs], ng + other[outs:]
    pg = (cg + row_back(ng, normed, factor)) / POOL
    pg = jnp.where(me * outs + iota(pg.shape, 0) < total, pg, 0.0).astype(BF16)
    pgw = dot_nt(pg, out_w[...]).astype(BF16)
    lift = ((iota((length, far), 0) + POOL - 1) // POOL == iota((length, far), 1)).astype(F32).astype(BF16)
    g_all[pl.ds(0, rows), :] = (gcot[...] + dot(lift[:rows], pgw)).astype(BF16)
    delta = head_sum(g_all[pl.ds(0, rows), :].astype(F32) * att_ref[...].astype(F32))
    stats[pl.ds(HEADS, HEADS), :] = delta.T[:HEADS]
    moves = [
        Shift(stats, stats_after.at[d - 1], stat_sems.at[0, d - 1], stat_sems.at[1, d - 1], -d)
        for d in range(1, hops + 1)
    ]
    for move in moves:
        move.start()
    up.stage(1)
    state = (pooled_own[:outs] + mixed).astype(BF16)
    onto = (iota((rows, outs), 0) // POOL == iota((rows, outs), 1)).astype(F32).astype(BF16)
    output_ref[...] = (hidden_ref[...].astype(F32) + dot(onto, state)).astype(BF16)
    for p in range(HEADS // 2):
        cols = pl.ds(p * PAIR, PAIR)
        dp = dot_nt(both(g_all[pl.ds(0, rows), cols]), v_all[:, cols])
        column = jnp.concatenate([delta[:, 2 * p : 2 * p + 1], delta[:, 2 * p + 1 : 2 * p + 2]])
        ds = (e_ref[p].astype(F32) * (dp - column)).astype(BF16)
        dq_ref[:, cols] = pick(dot(ds, k_all[:, cols]) * rt_ref[p]) * SCALE
    dq = head_back(dq_ref[...], unit_q[...], scale_q[...]).astype(BF16)
    dq_ref[...] = dot_nt(dq, w_ref[0])
    up_cot.stage(2)
    later = dot_nt(cot_after[...].reshape(margin, D), out_w[...])
    g_all[pl.ds(rows, margin), :] = (later + dot(lift[rows:], pgw)).astype(BF16)
    up.stage(2)
    for move in moves:
        move.wait()
    gap = iota((rows, length), 1) - iota((rows, length), 0)
    mask_t = (gap >= 0) & (gap < WINDOW)
    every = jnp.concatenate([stats[...]] + [stats_after[d] for d in range(hops)], axis=1)
    dk_p, dv_p = [], []
    for p in range(HEADS // 2):
        cols = pl.ds(p * PAIR, PAIR)
        own_slot = pl.ds(margin, rows)
        qp, gp = q_all[:, :, cols].reshape(length, PAIR), g_all[:, cols]
        st = dot_nt(both(k_all[own_slot, cols]), qp)
        dpt = dot_nt(both(v_all[own_slot, cols]), gp)
        pts, dsts = [], []
        for h in range(2):
            head = 2 * p + h
            part = slice(h * rows, (h + 1) * rows)
            pt = jnp.where(mask_t, jnp.exp2(st[part] - every[head : head + 1]), 0.0)
            pts.append(pt.astype(BF16))
            dsts.append((pt * (dpt[part] - every[HEADS + head : HEADS + head + 1])).astype(BF16))
        dk_p.append(pick(dot(jnp.concatenate(dsts), qp)) * LN2)
        dv_p.append(pick(dot(jnp.concatenate(pts), gp)))
    join = lambda parts: jnp.concatenate(parts, axis=1)
    dk = head_back(join(dk_p), unit_k[...], scale_k[...]).astype(BF16)
    dv = join(dv_p).astype(BF16)
    grads = dq_ref[...] + dot_nt(dk, w_ref[1]) + dot_nt(dv, w_ref[2])
    normed, factor = rms_rows(x_ref[...].astype(F32))
    hidden_grad = cot_ref[...].astype(F32) + dot(lift[:rows], pg)
    grad_ref[...] = (hidden_grad + row_back(grads, normed, factor)).astype(BF16)
    down.drain()
    up_cot.drain()
    up.drain()


def per_device(tokens, cotangent, fine_qkv, fine_out, coarse_qkv, coarse_out):
    rows = tokens.shape[0]
    hops = -(-WINDOW // rows)
    outs = rows // POOL
    me, count, subs = place()
    far = (hops + 2) * outs
    length = (hops + 1) * rows
    total = count * outs
    span = (subs - 1) * outs + far
    width = coarse_qkv.shape[2]
    pairs = HEADS // 2
    shape = jax.ShapeDtypeStruct
    dma = pltpu.SemaphoreType.DMA
    vmem = pltpu.VMEM
    fine_w = jnp.transpose(fine_qkv, (1, 0, 2))
    coarse_w = jnp.transpose(coarse_qkv, (1, 0, 2))
    wide = D + D // outs
    padded = total + far
    scratch = [
        vmem((rows, D), BF16), vmem((rows, D), BF16),
        vmem(fine_w.shape, BF16), vmem(fine_out.shape, BF16), vmem(coarse_w.shape, BF16),
        vmem(coarse_out.shape, BF16),
        vmem((hops, rows, D), BF16), vmem((hops + 1, rows, D), BF16), vmem((hops, rows, D), BF16),
        vmem((length, D), BF16), vmem((length, D), BF16),
        vmem((rows, D), F32), vmem((rows, D), F32), vmem((rows, D), F32), vmem((rows, D), F32),
        vmem((pairs, 2 * rows, length), BF16), vmem((pairs, 2 * rows, rows), F32),
        vmem((pairs, 2 * rows, PAIR), F32), vmem((pairs, 2 * rows, PAIR), F32),
        vmem((rows, D), BF16), vmem((rows, D), BF16),
        vmem((outs, D), BF16), vmem((count + far // outs, outs, D), BF16),
        vmem((outs, wide), BF16), vmem((count, outs, wide), BF16),
        vmem((padded, D), F32), vmem((rows, D), F32), vmem((length, D), BF16),
    ] + [vmem((padded, width), F32)] * 6 + [
        vmem((subs * outs, D), F32), vmem((span, D), F32),
        vmem((subs, outs + far, D), BF16), vmem((subs, outs + far, D), BF16),
        vmem((2 * HEADS, rows), F32), vmem((hops, 2 * HEADS, rows), F32), vmem((rows, D), F32),
        dma((8,)), *halo_sems(hops, 3), dma((2, subs)), dma((2, hops)),
    ] + spread_sems(count, subs) * 2
    return pl.pallas_call(
        functools.partial(layer_pair, hops),
        out_shape=[shape((rows, D), BF16)] * 2,
        in_specs=[HBM] * 6,
        out_specs=[VMEM] * 2,
        scratch_shapes=scratch,
        compiler_params=pltpu.CompilerParams(
            collective_id=0, has_side_effects=True, vmem_limit_bytes=(48 if total <= 1024 else 63) * 1024 * 1024
        ),
    )(*[
        pltpu.with_memory_space_constraint(a, pltpu.HBM)
        for a in (tokens, cotangent, fine_w, fine_out, coarse_w, coarse_out)
    ])


def solution(mesh):
    placed = (
        P(("seq", "sub"), None),
        P(("seq", "sub"), None),
        P(),
        P(),
        P(None, None, "sub"),
        P("sub", None),
    )
    return jax.shard_map(
        per_device,
        mesh=mesh,
        in_specs=placed,
        out_specs=(P(("seq", "sub"), None), P(("seq", "sub"), None)),
        check_vma=False,
    )
```
